256 devices in a mesh: gy: 8 (over z), gz: 32 (over x, y, core).
Axes of the slice: x: 4, y: 4, z: 8, core: 2. Of those that a mesh axis runs over, the one named last changes fastest.
Arguments:
- data_weight: float32 [640, 640, 640], P('gy', 'gz'), may hold values from 0.25 to 4
- blob_taps: float32 [3, 7], replicated, may hold values from 0.2 to 1
Outputs:
- new_weight: float32 [640, 640, 640], P('gy', 'gz')
- changes: float32 [3], replicated
The draws below stay inside these ranges and needn't reach their ends.
All inputs are finite; a program needn't handle non-finite values.
Results may differ from the reference program's by a relative error of at most 0.00002.
Values sent between devices are 32-bit elements; how exact they have to be, the bound alone decides.
A program may use at most 64 MiB of HBM per device.

```python
import math
import jax
import jax.numpy as jnp
from jax import lax

XLEN = 640
RAD = 3
TAPS = 7
ITERS = 3
YLEN = 640
ZLEN = 640


def level_of(key, extent, shards, least, largest):
    gain = 1.0
    for axis_at, parts in shards:
        heights = jax.random.uniform(jax.random.fold_in(jax.random.fold_in(key, 6), axis_at), (parts,), jnp.float32, least / len(shards), largest / len(shards))
        gain = gain * jnp.repeat(jnp.exp(heights), extent[axis_at] // parts).reshape((-1,) + (1,) * (len(extent) - 1 - axis_at))
    return gain


def setup_inputs(seed: int = 0) -> dict:
    arg_keys = jax.random.split(jax.random.key(seed), 3)
    return {
        "data_weight": jnp.clip(jnp.exp(math.log(4.0) - 2.7725887 * jax.random.uniform(arg_keys[0], (YLEN, ZLEN, XLEN), jnp.float32) ** level_of(arg_keys[0], (YLEN, ZLEN, XLEN), ((0, 8), (1, 32)), -0.2, 0.2)), 0.25, 4.0),
        "blob_taps": jnp.clip(jax.random.uniform(arg_keys[1], (3, TAPS), jnp.float32, 0.2, 1.0), 0.2, 1.0),
    }


def smear_axis(field, kernel, axis_dim):
    length = field.shape[axis_dim]
    widths = [(0, 0), (0, 0), (0, 0)]
    widths[axis_dim] = (RAD, RAD)
    padded = jnp.pad(field, widths)
    result = jnp.zeros_like(field)
    for offset in range(2 * RAD + 1):
        result = result + kernel[offset] * lax.slice_in_dim(padded, offset, offset + length, axis=axis_dim)
    return result


def reference(data_weight, blob_taps):
    kernel = blob_taps / jnp.sum(blob_taps, axis=1, keepdims=True)
    weight = jnp.ones_like(data_weight)
    changes = []
    for iteration in range(ITERS):
        product = weight * data_weight
        blurred = smear_axis(product, kernel[2], 2)
        blurred = smear_axis(blurred, kernel[0], 0)
        blurred = smear_axis(blurred, kernel[1], 1)
        weight = weight / blurred
        changes.append(jnp.max(jnp.abs(blurred - 1.0)))
    return weight, jnp.stack(changes)
```

```python
import functools

import jax
import jax.numpy as jnp
from jax import lax
from jax.experimental import pallas as pl
from jax.experimental.pallas import tpu as pltpu
from jax.sharding import PartitionSpec as P

MESH = pl.DeviceIdType.MESH
F32 = jnp.float32
BF16 = jnp.bfloat16

NZ, NY, NX = 20, 80, 640
DEEP = 9
G = 4
ROWS = 96
XR = 104
Y_GROUPS = ((0, 7), (7, 11), (11, 15), (15, 20), (20, 23), (23, 27), (27, 29))
X_GROUPS = ((0, 20, 0, 24), (20, 23, 24, 8), (23, 27, 32, 8), (27, 29, 40, 8))
XS = 48
TINY = 1e-30
X_BLOCKS = ((0, 256, 0, 384), (256, 256, 128, 512), (512, 128, 384, 256))


def split(v):
    hi = v.astype(BF16)
    return hi, (v - hi.astype(F32)).astype(BF16)


def kernel(
    dw, taps, out, dev_out, p1, p2, p3, q, rh, rl, w0, w1, w2, ay, ob, stat, sx, rx,
    load_sem, out_sem, oss, osr, yss, ysr, xss, xsr, iss, isr,
):
    gy, gz = lax.axis_index("gy"), lax.axis_index("gz")
    ny, nz = lax.axis_size("gy"), lax.axis_size("gz")
    core = lax.rem(gz, 2)
    inner = gz + 1 - 2 * core
    outer = gz - 1 + 2 * core
    has_outer = jnp.logical_and(outer >= 0, outer < nz)
    has_up = gy < ny - 1
    has_down = gy > 0

    def plane(s):
        return core * s + (1 - core) * (NZ - 1 - s)

    loads = [
        pltpu.make_async_copy(dw.at[plane(s)], p1.at[s + 3, 0:NY], load_sem.at[s]) for s in range(NZ)
    ]
    for copy in loads:
        copy.start()

    barrier = pltpu.get_barrier_semaphore()
    pl.semaphore_signal(barrier, inc=1, device_id={"gz": inner}, device_id_type=MESH)

    @pl.when(has_outer)
    def _():
        pl.semaphore_signal(barrier, inc=1, device_id={"gz": outer}, device_id_type=MESH)

    @pl.when(has_up)
    def _():
        pl.semaphore_signal(barrier, inc=1, device_id={"gy": gy + 1}, device_id_type=MESH)

    @pl.when(has_down)
    def _():
        pl.semaphore_signal(barrier, inc=1, device_id={"gy": gy - 1}, device_id_type=MESH)

    p1[3:34, ROWS:XR, :] = jnp.zeros((31, XR - ROWS, NX), F32)
    p1[32:34, 0:ROWS, :] = jnp.zeros((2, ROWS, NX), F32)

    @pl.when(jnp.logical_not(has_up))
    def _():
        p1[3:32, 80:88, :] = jnp.zeros((29, 8, NX), F32)
        rx[1] = jnp.zeros((XS, NX), F32)

    @pl.when(jnp.logical_not(has_down))
    def _():
        p1[3:32, 88:96, :] = jnp.zeros((29, 8, NX), F32)
        rx[0] = jnp.zeros((XS, NX), F32)

    @pl.when(jnp.logical_not(has_outer))
    def _():
        def clear(i, carry):
            p1[23 + i, 0:ROWS, :] = jnp.zeros((ROWS, NX), F32)
            return carry

        lax.fori_loop(0, DEEP, clear, 0)
        rx[0, 24:XS, :] = jnp.zeros((XS - 24, NX), F32)
        rx[1, 24:XS, :] = jnp.zeros((XS - 24, NX), F32)

    pl.semaphore_wait(
        barrier, 1 + has_outer.astype(jnp.int32) + has_up.astype(jnp.int32) + has_down.astype(jnp.int32)
    )

    def remote(src, dst, ss, rs, where):
        return pltpu.make_async_remote_copy(
            src_ref=src, dst_ref=dst, send_sem=ss, recv_sem=rs, device_id=where, device_id_type=MESH
        )

    outs = [
        remote(dw.at[plane(19 - i)], p1.at[23 + i, 0:NY], oss.at[i], osr.at[i], {"gz": outer})
        for i in range(DEEP)
    ]

    @pl.when(has_outer)
    def _():
        for copy in outs:
            copy.start()

    inner_own = [
        remote(dw.at[plane(i)], p1.at[2 - i, 0:NY], iss.at[i], isr.at[i], {"gz": inner}) for i in range(3)
    ]
    for copy in inner_own:
        copy.start()

    def y_copies(n):
        a, b = Y_GROUPS[n]
        pa, pb = a + 3, b + 3
        up = remote(p1.at[pa:pb, 72:80], p1.at[pa:pb, 88:96], yss.at[0, n], ysr.at[0, n], {"gy": gy + 1})
        down = remote(p1.at[pa:pb, 0:8], p1.at[pa:pb, 80:88], yss.at[1, n], ysr.at[1, n], {"gy": gy - 1})
        return up, down

    def x_copies(n):
        _, _, slot, size = X_GROUPS[n]
        at = slice(slot, slot + size)
        up = remote(sx.at[0, at], rx.at[0, at], xss.at[0, n], xsr.at[0, n], {"gy": gy + 1})
        down = remote(sx.at[1, at], rx.at[1, at], xss.at[1, n], xsr.at[1, n], {"gy": gy - 1})
        return up, down

    def start_y(n):
        up, down = y_copies(n)

        @pl.when(has_up)
        def _():
            up.start()

        @pl.when(has_down)
        def _():
            down.start()

    def start_x(n):
        a, b, slot, size = X_GROUPS[n]
        for i in range(size):
            s = min(a + i, b - 1)
            sx[0, slot + i : slot + i + 1, :] = p1[s + 3, 71:72, :]
            sx[1, slot + i : slot + i + 1, :] = p1[s + 3, 8:9, :]
        up, down = x_copies(n)

        @pl.when(has_up)
        def _():
            up.start()

        @pl.when(has_down)
        def _():
            down.start()

    def wait_y(n):
        up, down = y_copies(n)

        @pl.when(has_down)
        def _():
            up.wait_recv()

        @pl.when(has_up)
        def _():
            down.wait_recv()

    def wait_x(n):
        up, down = x_copies(n)

        @pl.when(has_down)
        def _():
            up.wait_recv()

        @pl.when(has_up)
        def _():
            down.wait_recv()

        a, b, slot, size = X_GROUPS[n]
        for i in range(b - a):
            p1[a + i + 3, 96:97, :] = rx[0, slot + i : slot + i + 1, :]
            p1[a + i + 3, 97:98, :] = rx[1, slot + i : slot + i + 1, :]

    for n in range(4):
        for s in range(*Y_GROUPS[n]):
            loads[s].wait()
        start_y(n)
    start_x(0)

    tv = taps[...]
    tv = tv / jnp.sum(tv, axis=1, keepdims=True)
    flip = core == 0
    kz = [jnp.where(flip, tv[1:2, 6 - k : 7 - k], tv[1:2, k : k + 1]) for k in range(7)]

    i = lax.broadcasted_iota(jnp.int32, (128, 128), 0)
    j = lax.broadcasted_iota(jnp.int32, (128, 128), 1)
    blocks = {}
    for delta in (-1, 0, 1):
        diff = delta * 128 + i - j + 3
        t = jnp.zeros((128, 128), F32)
        for k in range(7):
            t = jnp.where(diff == k, tv[2:3, k : k + 1], t)
        blocks[delta] = split(t)
    zero = jnp.zeros((128, 128), BF16)
    for w, (n0, nn, k0, kn) in zip((w0, w1, w2), X_BLOCKS):
        for part in range(3):
            for kb in range(kn // 128):
                for nb in range(nn // 128):
                    delta = (k0 // 128 + kb) - (n0 // 128 + nb)
                    block = blocks[delta][1 if part == 2 else 0] if abs(delta) <= 1 else zero
                    w[part * kn + kb * 128 : part * kn + (kb + 1) * 128, nb * 128 : (nb + 1) * 128] = block

    o = lax.broadcasted_iota(jnp.int32, (ROWS, 128), 0)
    i = lax.broadcasted_iota(jnp.int32, (ROWS, 128), 1)
    yo = jnp.where(o < 88, o, o - 96)
    yi = jnp.where(i < 88, i, jnp.where(i < 96, i - 96, jnp.where(i == 96, -9, jnp.where(i == 97, 88, 4096))))
    diff = yi - yo + 3
    t = jnp.zeros((ROWS, 128), F32)
    for k in range(7):
        t = jnp.where(diff == k, tv[0:1, k : k + 1], t)
    t_hi, t_lo = split(t)
    ay[0:ROWS, 0:128] = t_hi
    ay[0:ROWS, 128:256] = t_hi
    ay[ROWS : 2 * ROWS, 0:128] = t_lo
    ay[ROWS : 2 * ROWS, 128:256] = jnp.zeros((ROWS, 128), BF16)

    for g in range(G):
        q[g, 96:128, :] = jnp.zeros((32, NX), BF16)
        q[g, 224:256, :] = jnp.zeros((32, NX), BF16)
    for t in range(3):
        stat[t, 0] = jnp.zeros((8, 128), F32)
        stat[t, 1] = jnp.full((8, 128), 3e38, F32)

    def chunk(t, d):
        src = (p1, p2, p3)[t]
        base = d * G
        strips = 7 if t == 0 else 6
        for strip in range(strips):
            r0 = strip * 16
            height = 8 if strip == 6 else 16
            for lb in range(5):
                lanes = slice(lb * 128, (lb + 1) * 128)
                p = [src[base + k, r0 : r0 + height, lanes] for k in range(G + 6)]
                for g in range(G):
                    acc = kz[0] * p[g]
                    for k in range(1, 7):
                        acc = acc + kz[k] * p[g + k]
                    if height == 8:
                        acc = jnp.concatenate([acc, jnp.zeros((8, 128), F32)], axis=0)
                    hi, lo = split(acc)
                    q[g, r0 : r0 + 16, lanes] = hi
                    q[g, 128 + r0 : 144 + r0, lanes] = lo
        rows = 80 if t == 2 else ROWS
        for g in range(G):
            if t == 2:
                y = jnp.dot(ay[0:80, :], q[g], preferred_element_type=F32) + jnp.dot(
                    ay[ROWS : ROWS + 80, :], q[g], preferred_element_type=F32
                )
            else:
                y = jnp.dot(ay[...], q[g], preferred_element_type=F32)
                y = y[0:ROWS] + y[ROWS : 2 * ROWS]
            hi, lo = split(y)
            rh[g * rows : (g + 1) * rows, :] = hi
            rl[g * rows : (g + 1) * rows, :] = lo
        m = G * rows
        top = jnp.zeros((8, 128), F32)
        low = jnp.full((8, 128), 3e38, F32)
        for w, (n0, nn, k0, kn) in zip((w0, w1, w2), X_BLOCKS):
            hi, lo = rh[0:m, k0 : k0 + kn], rl[0:m, k0 : k0 + kn]
            b = jnp.dot(jnp.concatenate([hi, lo, hi], axis=1), w[...], preferred_element_type=F32)
            for g in range(G):
                for r0 in range(0, rows, 16):
                    for lb in range(nn // 128):
                        v = b[g * rows + r0 : g * rows + r0 + 16, lb * 128 : (lb + 1) * 128]
                        lanes = slice(n0 + lb * 128, n0 + (lb + 1) * 128)
                        if r0 < 80:
                            top = jnp.maximum(top, jnp.maximum(v[0:8], v[8:16]))
                            low = jnp.minimum(low, jnp.minimum(v[0:8], v[8:16]))
                        p = src[base + 3 + g, r0 : r0 + 16, lanes]
                        if t == 2:
                            f = p1[base + 3 + g, r0 : r0 + 16, lanes]
                            ob[base + g, r0 : r0 + 16, lanes] = p / (v * f)
                        else:
                            dst = (p2, p3)[t]
                            dst[base + 3 + g, r0 : r0 + 16, lanes] = p / jnp.maximum(v, TINY)
        own = d * G < NZ
        stat[t, 0] = jnp.where(own, jnp.maximum(stat[t, 0], top), stat[t, 0])
        stat[t, 1] = jnp.where(own, jnp.minimum(stat[t, 1], low), stat[t, 1])

    inner_rim = [
        remote(p1.at[3 + i, NY:XR], p1.at[2 - i, NY:XR], iss.at[3 + i], isr.at[3 + i], {"gz": inner})
        for i in range(3)
    ]
    inner_p2 = [
        remote(p2.at[3 + i], p2.at[2 - i], iss.at[6 + i], isr.at[6 + i], {"gz": inner}) for i in range(3)
    ]
    inner_p3 = [
        remote(p3.at[3 + i], p3.at[2 - i], iss.at[9 + i], isr.at[9 + i], {"gz": inner}) for i in range(3)
    ]
    outputs = lambda c: [
        pltpu.make_async_copy(ob.at[c * G + g], out.at[plane(c * G + g)], out_sem.at[c * G + g]) for g in range(G)
    ]

    def forward(n):
        a, b = Y_GROUPS[n]
        for s in range(a, b):
            outs[s - 20].wait_recv()
        start_y(n)
        start_x(n - 3)

    def wave(d, carry):
        @pl.when(d == 0)
        def _():
            wait_x(0)
            wait_y(0)
            for copy in inner_rim:
                copy.start()
            for copy in inner_own + inner_rim:
                copy.wait_recv()

        for n in (1, 2, 3):

            @pl.when(d == n)
            def _(n=n):
                wait_y(n)

        for n in (4, 5, 6):

            @pl.when(jnp.logical_and(d == n, has_outer))
            def _(n=n):
                wait_y(n)
                wait_x(n - 3)

        chunk(0, d)

        @pl.when(d == 0)
        def _():
            for copy in inner_p2:
                copy.start()

        for n in (4, 5, 6):

            @pl.when(jnp.logical_and(d == n - 1, has_outer))
            def _(n=n):
                forward(n)

        @pl.when(d == 1)
        def _():
            for copy in inner_p2:
                copy.wait_recv()

        @pl.when(d >= 1)
        def _():
            chunk(1, d - 1)

        @pl.when(d == 1)
        def _():
            for copy in inner_p3:
                copy.start()

        @pl.when(d == 2)
        def _():
            for copy in inner_p3:
                copy.wait_recv()

        @pl.when(d >= 2)
        def _():
            chunk(2, d - 2)
            for g in range(G):
                s = (d - 2) * G + g
                pltpu.make_async_copy(ob.at[s], out.at[plane(s)], out_sem.at[s]).start()

        return carry

    lax.fori_loop(0, 7, wave, 0)

    row = lax.broadcasted_iota(jnp.int32, (8, 128), 0)
    dev = jnp.zeros((8, 128), F32)
    for t in range(3):
        worst = jnp.maximum(jnp.max(stat[t, 0]) - 1.0, 1.0 - jnp.min(stat[t, 1]))
        dev = jnp.where(row == t, worst, dev)
    dev_out[...] = dev

    for s in range(NZ):
        pltpu.make_async_copy(ob.at[s], out.at[plane(s)], out_sem.at[s]).wait()
    for copy in inner_own + inner_rim + inner_p2 + inner_p3:
        copy.wait_send()

    @pl.when(has_outer)
    def _():
        for copy in outs:
            copy.wait_send()

    def sent(copies):
        up, down = copies

        @pl.when(has_up)
        def _():
            up.wait_send()

        @pl.when(has_down)
        def _():
            down.wait_send()

    for n in range(4):
        sent(y_copies(n))
    sent(x_copies(0))

    @pl.when(has_outer)
    def _():
        for n in (4, 5, 6):
            sent(y_copies(n))
            sent(x_copies(n - 3))


def shards(data_weight, blob_taps):
    dma = pltpu.SemaphoreType.DMA
    weight, dev = pl.pallas_call(
        kernel,
        out_shape=(
            jax.ShapeDtypeStruct((NZ, NY, NX), F32),
            jax.ShapeDtypeStruct((8, 128), F32),
        ),
        in_specs=[pl.BlockSpec(memory_space=pl.ANY), pl.BlockSpec(memory_space=pltpu.VMEM)],
        out_specs=(pl.BlockSpec(memory_space=pl.ANY), pl.BlockSpec(memory_space=pltpu.VMEM)),
        scratch_shapes=[
            pltpu.VMEM((34, XR, NX), F32),
            pltpu.VMEM((31, ROWS, NX), F32),
            pltpu.VMEM((27, ROWS, NX), F32),
            pltpu.VMEM((G, 256, NX), BF16),
            pltpu.VMEM((G * ROWS, NX), BF16),
            pltpu.VMEM((G * ROWS, NX), BF16),
            pltpu.VMEM((3 * 384, 256), BF16),
            pltpu.VMEM((3 * 512, 256), BF16),
            pltpu.VMEM((3 * 256, 128), BF16),
            pltpu.VMEM((2 * ROWS, 256), BF16),
            pltpu.VMEM((NZ, NY, NX), F32),
            pltpu.VMEM((3, 2, 8, 128), F32),
            pltpu.VMEM((2, XS, NX), F32),
            pltpu.VMEM((2, XS, NX), F32),
            dma((NZ,)),
            dma((NZ,)),
            dma((DEEP,)),
            dma((DEEP,)),
            dma((2, 7)),
            dma((2, 7)),
            dma((2, 4)),
            dma((2, 4)),
            dma((12,)),
            dma((12,)),
        ],
        compiler_params=pltpu.CompilerParams(
            collective_id=0, has_side_effects=True, vmem_limit_bytes=60 * 1024 * 1024
        ),
    )(jnp.transpose(data_weight, (1, 0, 2)), blob_taps)
    changes = lax.pmax(dev[:3, 0], ("gy", "gz"))
    return jnp.transpose(weight, (1, 0, 2)), changes


def solution(mesh):
    return jax.shard_map(
        shards,
        mesh=mesh,
        in_specs=(P("gy", "gz", None), P()),
        out_specs=(P("gy", "gz", None), P()),
        check_vma=False,
    )
```

```python
import functools

import jax
import jax.numpy as jnp
from jax import lax
from jax.experimental import pallas as pl
from jax.experimental.pallas import tpu as pltpu
from jax.sharding import PartitionSpec as P

MESH = pl.DeviceIdType.MESH
F32 = jnp.float32
BF16 = jnp.bfloat16

NZ, NY, NX = 20, 80, 640
DEEP = 9
G = 4
ROWS = 96
XR = 104
Y_GROUPS = ((0, 7), (7, 11), (11, 15), (15, 20), (20, 23), (23, 27), (27, 29))
X_GROUPS = ((0, 20, 0, 24), (20, 23, 24, 8), (23, 27, 32, 8), (27, 29, 40, 8))
XS = 48
TINY = 1e-30
REDUCE = ((8, 1, "gz"), (4, 8, "gz"), (8, 1, "gy"))
X_BLOCKS = ((0, 256, 0, 384), (256, 256, 128, 512), (512, 128, 384, 256))


def split(v):
    hi = v.astype(BF16)
    return hi, (v - hi.astype(F32)).astype(BF16)


def kernel(
    dw, taps, out, dev_out, p1, p2, p3, q, rh, rl, w0, w1, w2, ay, stat, sx, rx,
    mine, seen,
    load_sem, oss, osr, yss, ysr, xss, xsr, iss, isr, rds, rdr, met_z, met_y,
):
    gy, gz = lax.axis_index("gy"), lax.axis_index("gz")
    ny, nz = lax.axis_size("gy"), lax.axis_size("gz")
    core = lax.rem(gz, 2)
    inner = gz + 1 - 2 * core
    outer = gz - 1 + 2 * core
    has_outer = jnp.logical_and(outer >= 0, outer < nz)
    has_up = gy < ny - 1
    has_down = gy > 0

    def plane(s):
        return core * s + (1 - core) * (NZ - 1 - s)

    loads = [
        pltpu.make_async_copy(dw.at[plane(s)], p1.at[s + 3, 0:NY], load_sem.at[s]) for s in range(NZ)
    ]
    for copy in loads:
        copy.start()

    barrier = pltpu.get_barrier_semaphore()
    for axis, me, size in (("gz", gz, nz), ("gy", gy, ny)):
        for far in (1, size - 1):
            pl.semaphore_signal(barrier, inc=1, device_id={axis: lax.rem(me + far, size)}, device_id_type=MESH)

    p1[3:34, ROWS:XR, :] = jnp.zeros((31, XR - ROWS, NX), F32)
    p1[32:34, 0:ROWS, :] = jnp.zeros((2, ROWS, NX), F32)

    @pl.when(jnp.logical_not(has_up))
    def _():
        p1[3:32, 80:88, :] = jnp.zeros((29, 8, NX), F32)
        rx[1] = jnp.zeros((XS, NX), F32)

    @pl.when(jnp.logical_not(has_down))
    def _():
        p1[3:32, 88:96, :] = jnp.zeros((29, 8, NX), F32)
        rx[0] = jnp.zeros((XS, NX), F32)

    @pl.when(jnp.logical_not(has_outer))
    def _():
        def clear(i, carry):
            p1[23 + i, 0:ROWS, :] = jnp.zeros((ROWS, NX), F32)
            return carry

        lax.fori_loop(0, DEEP, clear, 0)
        rx[0, 24:XS, :] = jnp.zeros((XS - 24, NX), F32)
        rx[1, 24:XS, :] = jnp.zeros((XS - 24, NX), F32)

    pl.semaphore_wait(barrier, 4)

    def remote(src, dst, ss, rs, where):
        return pltpu.make_async_remote_copy(
            src_ref=src, dst_ref=dst, send_sem=ss, recv_sem=rs, device_id=where, device_id_type=MESH
        )

    outs = [
        remote(dw.at[plane(19 - i)], p1.at[23 + i, 0:NY], oss.at[i], osr.at[i], {"gz": outer})
        for i in range(DEEP)
    ]

    @pl.when(has_outer)
    def _():
        for copy in outs:
            copy.start()

    inner_own = [
        remote(dw.at[plane(i)], p1.at[2 - i, 0:NY], iss.at[i], isr.at[i], {"gz": inner}) for i in range(3)
    ]
    for copy in inner_own:
        copy.start()

    def y_copies(n):
        a, b = Y_GROUPS[n]
        pa, pb = a + 3, b + 3
        up = remote(p1.at[pa:pb, 72:80], p1.at[pa:pb, 88:96], yss.at[0, n], ysr.at[0, n], {"gy": gy + 1})
        down = remote(p1.at[pa:pb, 0:8], p1.at[pa:pb, 80:88], yss.at[1, n], ysr.at[1, n], {"gy": gy - 1})
        return up, down

    def x_copies(n):
        _, _, slot, size = X_GROUPS[n]
        at = slice(slot, slot + size)
        up = remote(sx.at[0, at], rx.at[0, at], xss.at[0, n], xsr.at[0, n], {"gy": gy + 1})
        down = remote(sx.at[1, at], rx.at[1, at], xss.at[1, n], xsr.at[1, n], {"gy": gy - 1})
        return up, down

    def start_y(n):
        up, down = y_copies(n)

        @pl.when(has_up)
        def _():
            up.start()

        @pl.when(has_down)
        def _():
            down.start()

    def start_x(n):
        a, b, slot, size = X_GROUPS[n]
        for i in range(size):
            s = min(a + i, b - 1)
            sx[0, slot + i : slot + i + 1, :] = p1[s + 3, 71:72, :]
            sx[1, slot + i : slot + i + 1, :] = p1[s + 3, 8:9, :]
        up, down = x_copies(n)

        @pl.when(has_up)
        def _():
            up.start()

        @pl.when(has_down)
        def _():
            down.start()

    def wait_y(n):
        up, down = y_copies(n)

        @pl.when(has_down)
        def _():
            up.wait_recv()

        @pl.when(has_up)
        def _():
            down.wait_recv()

    def wait_x(n):
        up, down = x_copies(n)

        @pl.when(has_down)
        def _():
            up.wait_recv()

        @pl.when(has_up)
        def _():
            down.wait_recv()

        a, b, slot, size = X_GROUPS[n]
        for i in range(b - a):
            p1[a + i + 3, 96:97, :] = rx[0, slot + i : slot + i + 1, :]
            p1[a + i + 3, 97:98, :] = rx[1, slot + i : slot + i + 1, :]

    for n in range(4):
        for s in range(*Y_GROUPS[n]):
            loads[s].wait()
        start_y(n)
    start_x(0)

    tv = taps[...]
    tv = tv / jnp.sum(tv, axis=1, keepdims=True)
    flip = core == 0
    kz = [jnp.where(flip, tv[1:2, 6 - k : 7 - k], tv[1:2, k : k + 1]) for k in range(7)]

    i = lax.broadcasted_iota(jnp.int32, (128, 128), 0)
    j = lax.broadcasted_iota(jnp.int32, (128, 128), 1)
    blocks = {}
    for delta in (-1, 0, 1):
        diff = delta * 128 + i - j + 3
        t = jnp.zeros((128, 128), F32)
        for k in range(7):
            t = jnp.where(diff == k, tv[2:3, k : k + 1], t)
        blocks[delta] = split(t)
    zero = jnp.zeros((128, 128), BF16)
    for w, (n0, nn, k0, kn) in zip((w0, w1, w2), X_BLOCKS):
        for part in range(3):
            for kb in range(kn // 128):
                for nb in range(nn // 128):
                    delta = (k0 // 128 + kb) - (n0 // 128 + nb)
                    block = blocks[delta][1 if part == 2 else 0] if abs(delta) <= 1 else zero
                    w[part * kn + kb * 128 : part * kn + (kb + 1) * 128, nb * 128 : (nb + 1) * 128] = block

    o = lax.broadcasted_iota(jnp.int32, (ROWS, 128), 0)
    i = lax.broadcasted_iota(jnp.int32, (ROWS, 128), 1)
    yo = jnp.where(o < 88, o, o - 96)
    yi = jnp.where(i < 88, i, jnp.where(i < 96, i - 96, jnp.where(i == 96, -9, jnp.where(i == 97, 88, 4096))))
    diff = yi - yo + 3
    t = jnp.zeros((ROWS, 128), F32)
    for k in range(7):
        t = jnp.where(diff == k, tv[0:1, k : k + 1], t)
    t_hi, t_lo = split(t)
    ay[0:ROWS, 0:128] = t_hi
    ay[0:ROWS, 128:256] = t_hi
    ay[ROWS : 2 * ROWS, 0:128] = t_lo
    ay[ROWS : 2 * ROWS, 128:256] = jnp.zeros((ROWS, 128), BF16)

    for g in range(G):
        q[g, 96:128, :] = jnp.zeros((32, NX), BF16)
        q[g, 224:256, :] = jnp.zeros((32, NX), BF16)
    for t in range(3):
        stat[t, 0] = jnp.zeros((8, 128), F32)
        stat[t, 1] = jnp.full((8, 128), 3e38, F32)

    def chunk(t, d):
        src = (p1, p2, p3)[t]
        base = d * G
        strips = 7 if t == 0 else 6
        for strip in range(strips):
            r0 = strip * 16
            height = 8 if strip == 6 else 16
            for lb in range(5):
                lanes = slice(lb * 128, (lb + 1) * 128)
                p = [src[base + k, r0 : r0 + height, lanes] for k in range(G + 6)]
                for g in range(G):
                    acc = kz[0] * p[g]
                    for k in range(1, 7):
                        acc = acc + kz[k] * p[g + k]
                    if height == 8:
                        acc = jnp.concatenate([acc, jnp.zeros((8, 128), F32)], axis=0)
                    hi, lo = split(acc)
                    q[g, r0 : r0 + 16, lanes] = hi
                    q[g, 128 + r0 : 144 + r0, lanes] = lo
        rows = 80 if t == 2 else ROWS
        for g in range(G):
            if t == 2:
                y = jnp.dot(ay[0:80, :], q[g], preferred_element_type=F32) + jnp.dot(
                    ay[ROWS : ROWS + 80, :], q[g], preferred_element_type=F32
                )
            else:
                y = jnp.dot(ay[...], q[g], preferred_element_type=F32)
                y = y[0:ROWS] + y[ROWS : 2 * ROWS]
            hi, lo = split(y)
            rh[g * rows : (g + 1) * rows, :] = hi
            rl[g * rows : (g + 1) * rows, :] = lo
        m = G * rows
        top = jnp.zeros((8, 128), F32)
        low = jnp.full((8, 128), 3e38, F32)
        for w, (n0, nn, k0, kn) in zip((w0, w1, w2), X_BLOCKS):
            hi, lo = rh[0:m, k0 : k0 + kn], rl[0:m, k0 : k0 + kn]
            b = jnp.dot(jnp.concatenate([hi, lo, hi], axis=1), w[...], preferred_element_type=F32)
            for g in range(G):
                for r0 in range(0, rows, 16):
                    for lb in range(nn // 128):
                        v = b[g * rows + r0 : g * rows + r0 + 16, lb * 128 : (lb + 1) * 128]
                        lanes = slice(n0 + lb * 128, n0 + (lb + 1) * 128)
                        if r0 < 80:
                            top = jnp.maximum(top, jnp.maximum(v[0:8], v[8:16]))
                            low = jnp.minimum(low, jnp.minimum(v[0:8], v[8:16]))
                        p = src[base + 3 + g, r0 : r0 + 16, lanes]
                        if t == 2:
                            f = p1[base + 3 + g, r0 : r0 + 16, lanes]
                            out[plane(base + g), r0 : r0 + 16, lanes] = p / (v * f)
                        else:
                            dst = (p2, p3)[t]
                            dst[base + 3 + g, r0 : r0 + 16, lanes] = p / jnp.maximum(v, TINY)
        own = d * G < NZ
        stat[t, 0] = jnp.where(own, jnp.maximum(stat[t, 0], top), stat[t, 0])
        stat[t, 1] = jnp.where(own, jnp.minimum(stat[t, 1], low), stat[t, 1])

    inner_rim = [
        remote(p1.at[3 + i, NY:XR], p1.at[2 - i, NY:XR], iss.at[3 + i], isr.at[3 + i], {"gz": inner})
        for i in range(3)
    ]
    inner_p2 = [
        remote(p2.at[3 + i], p2.at[2 - i], iss.at[6 + i], isr.at[6 + i], {"gz": inner}) for i in range(3)
    ]
    inner_p3 = [
        remote(p3.at[3 + i], p3.at[2 - i], iss.at[9 + i], isr.at[9 + i], {"gz": inner}) for i in range(3)
    ]
    def forward(n):
        a, b = Y_GROUPS[n]
        for s in range(a, b):
            outs[s - 20].wait_recv()
        start_y(n)
        start_x(n - 3)

    def meet(k, wait):
        far = 2**k
        for axis, me, size in (("gz", gz, nz), ("gy", gy, ny)):
            if 4 * far <= size:
                sem = (met_z if axis == "gz" else met_y).at[k]
                if wait:
                    pl.semaphore_wait(sem, 2)
                else:
                    for by in (far, size - far):
                        pl.semaphore_signal(
                            sem, inc=1, device_id={axis: lax.rem(me + by, size)}, device_id_type=MESH
                        )

    def wave(d, carry):
        for k in range(5):

            @pl.when(d == k)
            def _(k=k):
                if k > 0:
                    meet(k - 1, True)
                if k < 4:
                    meet(k, False)

        @pl.when(d == 0)
        def _():
            wait_x(0)
            wait_y(0)
            for copy in inner_rim:
                copy.start()
            for copy in inner_own + inner_rim:
                copy.wait_recv()

        for n in (1, 2, 3):

            @pl.when(d == n)
            def _(n=n):
                wait_y(n)

        for n in (4, 5, 6):

            @pl.when(jnp.logical_and(d == n, has_outer))
            def _(n=n):
                wait_y(n)
                wait_x(n - 3)

        chunk(0, d)

        @pl.when(d == 0)
        def _():
            for copy in inner_p2:
                copy.start()

        for n in (4, 5, 6):

            @pl.when(jnp.logical_and(d == n - 1, has_outer))
            def _(n=n):
                forward(n)

        @pl.when(d == 1)
        def _():
            for copy in inner_p2:
                copy.wait_recv()

        @pl.when(d >= 1)
        def _():
            chunk(1, d - 1)

        @pl.when(d == 1)
        def _():
            for copy in inner_p3:
                copy.start()

        @pl.when(d == 2)
        def _():
            for copy in inner_p3:
                copy.wait_recv()

        @pl.when(d >= 2)
        def _():
            chunk(2, d - 2)

        return carry

    lax.fori_loop(0, 7, wave, 0)

    lane = lax.broadcasted_iota(jnp.int32, (1, 128), 1)
    dev = jnp.zeros((1, 128), F32)
    for t in range(3):
        worst = jnp.maximum(jnp.max(stat[t, 0]) - 1.0, 1.0 - jnp.min(stat[t, 1]))
        dev = jnp.where(lane == t, worst, dev)

    value = dev
    for stage, (size, stride, axis) in enumerate(REDUCE):
        me = gy if axis == "gy" else gz
        member = lax.rem(me // stride, size)
        seen[stage, member] = value
        mine[stage] = value

        def copy(k):
            other = lax.rem(member + k, size)
            return remote(
                mine.at[stage], seen.at[stage, member], rds.at[stage, k], rdr.at[stage, member],
                {axis: me + (other - member) * stride},
            )

        def arrival(k):
            other = lax.rem(member + k, size)
            return remote(
                mine.at[stage], seen.at[stage, other], rds.at[stage, k], rdr.at[stage, other],
                {axis: me + (other - member) * stride},
            )

        for k in range(1, size):
            copy(k).start()
        for k in range(1, size):
            arrival(k).wait_recv()
        value = jnp.max(seen[stage, 0:size], axis=0)
    for stage, (size, stride, axis) in enumerate(REDUCE):
        me = gy if axis == "gy" else gz
        member = lax.rem(me // stride, size)
        for k in range(1, size):
            other = lax.rem(member + k, size)
            remote(
                mine.at[stage], seen.at[stage, member], rds.at[stage, k], rdr.at[stage, member],
                {axis: me + (other - member) * stride},
            ).wait_send()
    dev = value
    dev_out[...] = dev

    for copy in inner_own + inner_rim + inner_p2 + inner_p3:
        copy.wait_send()

    @pl.when(has_outer)
    def _():
        for copy in outs:
            copy.wait_send()

    def sent(copies):
        up, down = copies

        @pl.when(has_up)
        def _():
            up.wait_send()

        @pl.when(has_down)
        def _():
            down.wait_send()

    for n in range(4):
        sent(y_copies(n))
    sent(x_copies(0))

    @pl.when(has_outer)
    def _():
        for n in (4, 5, 6):
            sent(y_copies(n))
            sent(x_copies(n - 3))


def shards(data_weight, blob_taps):
    dma = pltpu.SemaphoreType.DMA
    weight, dev = pl.pallas_call(
        kernel,
        out_shape=(
            jax.ShapeDtypeStruct((NZ, NY, NX), F32),
            jax.ShapeDtypeStruct((1, 128), F32),
        ),
        in_specs=[pl.BlockSpec(memory_space=pl.ANY), pl.BlockSpec(memory_space=pltpu.VMEM)],
        out_specs=(pl.BlockSpec(memory_space=pltpu.VMEM), pl.BlockSpec(memory_space=pltpu.VMEM)),
        scratch_shapes=[
            pltpu.VMEM((34, XR, NX), F32),
            pltpu.VMEM((31, ROWS, NX), F32),
            pltpu.VMEM((27, ROWS, NX), F32),
            pltpu.VMEM((G, 256, NX), BF16),
            pltpu.VMEM((G * ROWS, NX), BF16),
            pltpu.VMEM((G * ROWS, NX), BF16),
            pltpu.VMEM((3 * 384, 256), BF16),
            pltpu.VMEM((3 * 512, 256), BF16),
            pltpu.VMEM((3 * 256, 128), BF16),
            pltpu.VMEM((2 * ROWS, 256), BF16),
            pltpu.VMEM((3, 2, 8, 128), F32),
            pltpu.VMEM((2, XS, NX), F32),
            pltpu.VMEM((2, XS, NX), F32),
            pltpu.VMEM((len(REDUCE), 1, 128), F32),
            pltpu.VMEM((len(REDUCE), 8, 1, 128), F32),
            dma((NZ,)),
            dma((DEEP,)),
            dma((DEEP,)),
            dma((2, 7)),
            dma((2, 7)),
            dma((2, 4)),
            dma((2, 4)),
            dma((12,)),
            dma((12,)),
            dma((len(REDUCE), 8)),
            dma((len(REDUCE), 8)),
            pltpu.SemaphoreType.REGULAR((4,)),
            pltpu.SemaphoreType.REGULAR((2,)),
        ],
        compiler_params=pltpu.CompilerParams(
            collective_id=0, has_side_effects=True, vmem_limit_bytes=50 * 1024 * 1024
        ),
    )(jnp.transpose(data_weight, (1, 0, 2)), blob_taps)
    return jnp.transpose(weight, (1, 0, 2)), dev[0, :3]


def solution(mesh):
    return jax.shard_map(
        shards,
        mesh=mesh,
        in_specs=(P("gy", "gz", None), P()),
        out_specs=(P("gy", "gz", None), P()),
        check_vma=False,
    )
```

```python
import functools

import jax
import jax.numpy as jnp
from jax import lax
from jax.experimental import pallas as pl
from jax.experimental.pallas import tpu as pltpu
from jax.sharding import PartitionSpec as P

MESH = pl.DeviceIdType.MESH
F32 = jnp.float32
BF16 = jnp.bfloat16

NZ, NY, NX = 20, 80, 640
DEEP = 9
G = 4
ROWS = 96
XR = 104
Y_GROUPS = ((0, 7), (7, 11), (11, 15), (15, 20), (20, 23), (23, 27), (27, 29))
X_GROUPS = ((0, 7, 0, 8), (7, 20, 8, 16), (20, 23, 24, 8), (23, 27, 32, 8), (27, 29, 40, 8))
XS = 48
TINY = 1e-30
REDUCE = ((32, 1, "gz"), (8, 1, "gy"))
X_BLOCKS = ((0, 256, 0), (256, 256, 1), (512, 128, 0))


def split(v):
    hi = v.astype(BF16)
    return hi, (v - hi.astype(F32)).astype(BF16)


def kernel(
    dw, taps, out, dev_out, p1, p2, p3, q, rh, rl, edge, w0, w1, w2, ay, stat, sx, rx,
    mine, seen,
    load_sem, oss, osr, yss, ysr, xss, xsr, iss, isr, rds, rdr, met_z, met_y,
):
    gy, gz = lax.axis_index("gy"), lax.axis_index("gz")
    ny, nz = lax.axis_size("gy"), lax.axis_size("gz")
    core = lax.rem(gz, 2)
    inner = gz + 1 - 2 * core
    outer = gz - 1 + 2 * core
    has_outer = jnp.logical_and(outer >= 0, outer < nz)
    has_up = gy < ny - 1
    has_down = gy > 0

    def plane(s):
        return core * s + (1 - core) * (NZ - 1 - s)

    loads = [
        pltpu.make_async_copy(dw.at[plane(s)], p1.at[s + 3, 0:NY], load_sem.at[s]) for s in range(NZ)
    ]
    for copy in loads:
        copy.start()

    barrier = pltpu.get_barrier_semaphore()
    for axis, me, size in (("gz", gz, nz), ("gy", gy, ny)):
        for far in (1, size - 1):
            pl.semaphore_signal(barrier, inc=1, device_id={axis: lax.rem(me + far, size)}, device_id_type=MESH)

    p1[3:34, ROWS:XR, :] = jnp.zeros((31, XR - ROWS, NX), F32)
    p1[32:34, 0:ROWS, :] = jnp.zeros((2, ROWS, NX), F32)

    @pl.when(jnp.logical_not(has_up))
    def _():
        p1[3:32, 80:88, :] = jnp.zeros((29, 8, NX), F32)
        rx[1] = jnp.zeros((XS, NX), F32)

    @pl.when(jnp.logical_not(has_down))
    def _():
        p1[3:32, 88:96, :] = jnp.zeros((29, 8, NX), F32)
        rx[0] = jnp.zeros((XS, NX), F32)

    @pl.when(jnp.logical_not(has_outer))
    def _():
        def clear(i, carry):
            p1[23 + i, 0:ROWS, :] = jnp.zeros((ROWS, NX), F32)
            return carry

        lax.fori_loop(0, DEEP, clear, 0)
        rx[0, 24:XS, :] = jnp.zeros((XS - 24, NX), F32)
        rx[1, 24:XS, :] = jnp.zeros((XS - 24, NX), F32)

    pl.semaphore_wait(barrier, 4)

    def remote(src, dst, ss, rs, where):
        return pltpu.make_async_remote_copy(
            src_ref=src, dst_ref=dst, send_sem=ss, recv_sem=rs, device_id=where, device_id_type=MESH
        )

    outs = [
        remote(dw.at[plane(19 - i)], p1.at[23 + i, 0:NY], oss.at[i], osr.at[i], {"gz": outer})
        for i in range(DEEP)
    ]

    inner_own = [
        remote(dw.at[plane(i)], p1.at[2 - i, 0:NY], iss.at[i], isr.at[i], {"gz": inner}) for i in range(3)
    ]
    def y_copies(n):
        a, b = Y_GROUPS[n]
        pa, pb = a + 3, b + 3
        up = remote(p1.at[pa:pb, 72:80], p1.at[pa:pb, 88:96], yss.at[0, n], ysr.at[0, n], {"gy": gy + 1})
        down = remote(p1.at[pa:pb, 0:8], p1.at[pa:pb, 80:88], yss.at[1, n], ysr.at[1, n], {"gy": gy - 1})
        return up, down

    def x_copies(n):
        _, _, slot, size = X_GROUPS[n]
        at = slice(slot, slot + size)
        up = remote(sx.at[0, at], rx.at[0, at], xss.at[0, n], xsr.at[0, n], {"gy": gy + 1})
        down = remote(sx.at[1, at], rx.at[1, at], xss.at[1, n], xsr.at[1, n], {"gy": gy - 1})
        return up, down

    def start_y(n):
        up, down = y_copies(n)

        @pl.when(has_up)
        def _():
            up.start()

        @pl.when(has_down)
        def _():
            down.start()

    def start_x(n):
        a, b, slot, size = X_GROUPS[n]
        for i in range(size):
            s = min(a + i, b - 1)
            sx[0, slot + i : slot + i + 1, :] = p1[s + 3, 71:72, :]
            sx[1, slot + i : slot + i + 1, :] = p1[s + 3, 8:9, :]
        up, down = x_copies(n)

        @pl.when(has_up)
        def _():
            up.start()

        @pl.when(has_down)
        def _():
            down.start()

    def wait_y(n):
        up, down = y_copies(n)

        @pl.when(has_down)
        def _():
            up.wait_recv()

        @pl.when(has_up)
        def _():
            down.wait_recv()

    def wait_x(n):
        up, down = x_copies(n)

        @pl.when(has_down)
        def _():
            up.wait_recv()

        @pl.when(has_up)
        def _():
            down.wait_recv()

        a, b, slot, size = X_GROUPS[n]
        for i in range(b - a):
            p1[a + i + 3, 96:97, :] = rx[0, slot + i : slot + i + 1, :]
            p1[a + i + 3, 97:98, :] = rx[1, slot + i : slot + i + 1, :]

    for s in range(7):
        loads[s].wait()
    start_x(0)
    start_y(0)

    @pl.when(has_outer)
    def _():
        for copy in outs:
            copy.start()

    for copy in inner_own:
        copy.start()

    for s in range(7, NZ):
        loads[s].wait()
    start_y(1)
    start_x(1)
    start_y(2)
    start_y(3)

    tv = taps[...]
    tv = tv / jnp.sum(tv, axis=1, keepdims=True)
    flip = core == 0
    kz = [jnp.where(flip, tv[1:2, 6 - k : 7 - k], tv[1:2, k : k + 1]) for k in range(7)]

    def banded(diff):
        t = jnp.zeros(diff.shape, F32)
        for k in range(7):
            t = jnp.where(diff == k - 3, tv[2:3, k : k + 1], t)
        return split(t)

    i = lax.broadcasted_iota(jnp.int32, (128, 128), 0)
    j = lax.broadcasted_iota(jnp.int32, (128, 128), 1)
    blocks = [banded(delta * 128 + i - j) for delta in (-1, 0, 1)]
    for w, (n0, nn, _) in zip((w0, w1, w2), X_BLOCKS):
        for part in range(3):
            for kb in range(nn // 128):
                for nb in range(nn // 128):
                    rows = slice(part * nn + kb * 128, part * nn + (kb + 1) * 128)
                    w[rows, nb * 128 : (nb + 1) * 128] = blocks[kb - nb + 1][part // 2]
        part = jnp.where(jnp.logical_or(i < 3, i >= 125), 0, jnp.where(i < 11, 1, 2))
        step = i - 8 * part
        step = jnp.where(step >= 125, step - 128, step)
        right = jnp.logical_and(step >= 0, step < (3 if n0 + nn < NX else 0))
        left = jnp.logical_and(step < 0, step >= (-3 if n0 > 0 else 0))
        for nb in range(nn // 128):
            out_lane = j + nb * 128
            diff = jnp.where(right, nn + step - out_lane, jnp.where(left, step - out_lane, 4096))
            hi, lo = banded(diff)
            w[3 * nn : 3 * nn + 128, nb * 128 : (nb + 1) * 128] = jnp.where(part == 2, lo.astype(F32), hi.astype(F32)).astype(BF16)

    o = lax.broadcasted_iota(jnp.int32, (ROWS, 128), 0)
    i = lax.broadcasted_iota(jnp.int32, (ROWS, 128), 1)
    yo = jnp.where(o < 88, o, o - 96)
    yi = jnp.where(i < 88, i, jnp.where(i < 96, i - 96, jnp.where(i == 96, -9, jnp.where(i == 97, 88, 4096))))
    diff = yi - yo + 3
    t = jnp.zeros((ROWS, 128), F32)
    for k in range(7):
        t = jnp.where(diff == k, tv[0:1, k : k + 1], t)
    t_hi, t_lo = split(t)
    ay[0:ROWS, 0:128] = t_hi
    ay[0:ROWS, 128:256] = t_hi
    ay[ROWS : 2 * ROWS, 0:128] = t_lo
    ay[ROWS : 2 * ROWS, 128:256] = jnp.zeros((ROWS, 128), BF16)

    for g in range(G):
        q[g, 96:128, :] = jnp.zeros((32, NX), BF16)
        q[g, 224:256, :] = jnp.zeros((32, NX), BF16)
    for t in range(3):
        stat[t, 0] = jnp.zeros((8, 128), F32)
        stat[t, 1] = jnp.full((8, 128), 3e38, F32)

    def chunk(t, d):
        src = (p1, p2, p3)[t]
        base = d * G
        strips = 7 if t == 0 else 6
        for strip in range(strips):
            r0 = strip * 16
            height = 8 if strip == 6 else 16
            for lb in range(5):
                lanes = slice(lb * 128, (lb + 1) * 128)
                p = [src[base + k, r0 : r0 + height, lanes] for k in range(G + 6)]
                for g in range(G):
                    acc = kz[0] * p[g]
                    for k in range(1, 7):
                        acc = acc + kz[k] * p[g + k]
                    if height == 8:
                        acc = jnp.concatenate([acc, jnp.zeros((8, 128), F32)], axis=0)
                    hi, lo = split(acc)
                    q[g, r0 : r0 + 16, lanes] = hi
                    q[g, 128 + r0 : 144 + r0, lanes] = lo
        rows = 80 if t == 2 else ROWS
        for g in range(G):
            if t == 2:
                y = jnp.dot(ay[0:80, :], q[g], preferred_element_type=F32) + jnp.dot(
                    ay[ROWS : ROWS + 80, :], q[g], preferred_element_type=F32
                )
            else:
                y = jnp.dot(ay[...], q[g], preferred_element_type=F32)
                y = y[0:ROWS] + y[ROWS : 2 * ROWS]
            hi, lo = split(y)
            at = slice(g * rows, (g + 1) * rows)
            rh[at, :] = hi
            rl[at, :] = lo
            lane = lax.broadcasted_iota(jnp.int32, (rows, 128), 1)
            for e, (after, ahead) in enumerate(((2, 3), (4, 1))):
                rim = jnp.where(
                    lane < 64, y[:, after * 128 : (after + 1) * 128], y[:, ahead * 128 : (ahead + 1) * 128]
                )
                rim_hi = rim.astype(BF16).astype(F32)
                rim = jnp.where(
                    jnp.logical_or(lane < 3, lane >= 125),
                    rim_hi,
                    jnp.where(lane < 11, pltpu.roll(rim - rim_hi, 8, 1), pltpu.roll(rim_hi, 16, 1)),
                )
                edge[e, at, :] = rim.astype(BF16)
        m = G * rows
        top = jnp.zeros((8, 128), F32)
        low = jnp.full((8, 128), 3e38, F32)
        for w, (n0, nn, e) in zip((w0, w1, w2), X_BLOCKS):
            hi, lo = rh[0:m, n0 : n0 + nn], rl[0:m, n0 : n0 + nn]
            b = jnp.dot(jnp.concatenate([hi, lo, hi, edge[e, 0:m]], axis=1), w[...], preferred_element_type=F32)
            for g in range(G):
                for r0 in range(0, rows, 16):
                    for lb in range(nn // 128):
                        v = b[g * rows + r0 : g * rows + r0 + 16, lb * 128 : (lb + 1) * 128]
                        lanes = slice(n0 + lb * 128, n0 + (lb + 1) * 128)
                        if r0 < 80:
                            top = jnp.maximum(top, jnp.maximum(v[0:8], v[8:16]))
                            low = jnp.minimum(low, jnp.minimum(v[0:8], v[8:16]))
                        p = src[base + 3 + g, r0 : r0 + 16, lanes]
                        if t == 2:
                            f = p1[base + 3 + g, r0 : r0 + 16, lanes]
                            out[plane(base + g), r0 : r0 + 16, lanes] = p / (v * f)
                        else:
                            dst = (p2, p3)[t]
                            dst[base + 3 + g, r0 : r0 + 16, lanes] = p / jnp.maximum(v, TINY)
        own = d * G < NZ
        stat[t, 0] = jnp.where(own, jnp.maximum(stat[t, 0], top), stat[t, 0])
        stat[t, 1] = jnp.where(own, jnp.minimum(stat[t, 1], low), stat[t, 1])

    inner_rim = [
        remote(p1.at[3 + i, NY:XR], p1.at[2 - i, NY:XR], iss.at[3 + i], isr.at[3 + i], {"gz": inner})
        for i in range(3)
    ]
    inner_p2 = [
        remote(p2.at[3 + i], p2.at[2 - i], iss.at[6 + i], isr.at[6 + i], {"gz": inner}) for i in range(3)
    ]
    inner_p3 = [
        remote(p3.at[3 + i], p3.at[2 - i], iss.at[9 + i], isr.at[9 + i], {"gz": inner}) for i in range(3)
    ]
    def forward(n):
        a, b = Y_GROUPS[n]
        for s in range(a, b):
            outs[s - 20].wait_recv()
        start_y(n)
        start_x(n - 2)

    def meet(k, wait):
        far = 2**k
        for axis, me, size in (("gz", gz, nz), ("gy", gy, ny)):
            if 4 * far <= size:
                sem = (met_z if axis == "gz" else met_y).at[k]
                if wait:
                    pl.semaphore_wait(sem, 2)
                else:
                    for by in (far, size - far):
                        pl.semaphore_signal(
                            sem, inc=1, device_id={axis: lax.rem(me + by, size)}, device_id_type=MESH
                        )

    def wave(d, carry):
        for k in range(5):

            @pl.when(d == k)
            def _(k=k):
                if k > 0:
                    meet(k - 1, True)
                if k < 4:
                    meet(k, False)

        @pl.when(d == 0)
        def _():
            wait_x(0)
            wait_y(0)
            for copy in inner_rim:
                copy.start()
            for copy in inner_own + inner_rim:
                copy.wait_recv()

        for n in (1, 2, 3):

            @pl.when(d == n)
            def _(n=n):
                wait_y(n)
                if n == 1:
                    wait_x(1)

        for n in (4, 5, 6):

            @pl.when(jnp.logical_and(d == n, has_outer))
            def _(n=n):
                wait_y(n)
                wait_x(n - 2)

        chunk(0, d)

        @pl.when(d == 0)
        def _():
            for copy in inner_p2:
                copy.start()

        for n in (4, 5, 6):

            @pl.when(jnp.logical_and(d == n - 1, has_outer))
            def _(n=n):
                forward(n)

        @pl.when(d == 1)
        def _():
            for copy in inner_p2:
                copy.wait_recv()

        @pl.when(d >= 1)
        def _():
            chunk(1, d - 1)

        @pl.when(d == 1)
        def _():
            for copy in inner_p3:
                copy.start()

        @pl.when(d == 2)
        def _():
            for copy in inner_p3:
                copy.wait_recv()

        @pl.when(d >= 2)
        def _():
            chunk(2, d - 2)

        return carry

    lax.fori_loop(0, 7, wave, 0)

    lane = lax.broadcasted_iota(jnp.int32, (1, 128), 1)
    dev = jnp.zeros((1, 128), F32)
    for t in range(3):
        worst = jnp.maximum(jnp.max(stat[t, 0]) - 1.0, 1.0 - jnp.min(stat[t, 1]))
        dev = jnp.where(lane == t, worst, dev)

    value = dev
    for stage, (size, stride, axis) in enumerate(REDUCE):
        me = gy if axis == "gy" else gz
        member = lax.rem(me // stride, size)
        seen[stage, member] = value
        mine[stage] = value

        def copy(k):
            other = lax.rem(member + k, size)
            return remote(
                mine.at[stage], seen.at[stage, member], rds.at[stage, k], rdr.at[stage, member],
                {axis: me + (other - member) * stride},
            )

        def arrival(k):
            other = lax.rem(member + k, size)
            return remote(
                mine.at[stage], seen.at[stage, other], rds.at[stage, k], rdr.at[stage, other],
                {axis: me + (other - member) * stride},
            )

        for k in range(1, size):
            copy(k).start()
        for k in range(1, size):
            arrival(k).wait_recv()
        value = jnp.max(seen[stage, 0:size], axis=0)
    for stage, (size, stride, axis) in enumerate(REDUCE):
        me = gy if axis == "gy" else gz
        member = lax.rem(me // stride, size)
        for k in range(1, size):
            other = lax.rem(member + k, size)
            remote(
                mine.at[stage], seen.at[stage, member], rds.at[stage, k], rdr.at[stage, member],
                {axis: me + (other - member) * stride},
            ).wait_send()
    dev = value
    dev_out[...] = dev

    for copy in inner_own + inner_rim + inner_p2 + inner_p3:
        copy.wait_send()

    @pl.when(has_outer)
    def _():
        for copy in outs:
            copy.wait_send()

    def sent(copies):
        up, down = copies

        @pl.when(has_up)
        def _():
            up.wait_send()

        @pl.when(has_down)
        def _():
            down.wait_send()

    for n in range(4):
        sent(y_copies(n))
    for n in range(2):
        sent(x_copies(n))

    @pl.when(has_outer)
    def _():
        for n in (4, 5, 6):
            sent(y_copies(n))
            sent(x_copies(n - 2))


def shards(data_weight, blob_taps):
    dma = pltpu.SemaphoreType.DMA
    weight, dev = pl.pallas_call(
        kernel,
        out_shape=(
            jax.ShapeDtypeStruct((NZ, NY, NX), F32),
            jax.ShapeDtypeStruct((1, 128), F32),
        ),
        in_specs=[pl.BlockSpec(memory_space=pl.ANY), pl.BlockSpec(memory_space=pltpu.VMEM)],
        out_specs=(pl.BlockSpec(memory_space=pltpu.VMEM), pl.BlockSpec(memory_space=pltpu.VMEM)),
        scratch_shapes=[
            pltpu.VMEM((34, XR, NX), F32),
            pltpu.VMEM((31, ROWS, NX), F32),
            pltpu.VMEM((27, ROWS, NX), F32),
            pltpu.VMEM((G, 256, NX), BF16),
            pltpu.VMEM((G * ROWS, NX), BF16),
            pltpu.VMEM((G * ROWS, NX), BF16),
            pltpu.VMEM((2, G * ROWS, 128), BF16),
            pltpu.VMEM((3 * 256 + 128, 256), BF16),
            pltpu.VMEM((3 * 256 + 128, 256), BF16),
            pltpu.VMEM((3 * 128 + 128, 128), BF16),
            pltpu.VMEM((2 * ROWS, 256), BF16),
            pltpu.VMEM((3, 2, 8, 128), F32),
            pltpu.VMEM((2, XS, NX), F32),
            pltpu.VMEM((2, XS, NX), F32),
            pltpu.VMEM((len(REDUCE), 1, 128), F32),
            pltpu.VMEM((len(REDUCE), 32, 1, 128), F32),
            dma((NZ,)),
            dma((DEEP,)),
            dma((DEEP,)),
            dma((2, 7)),
            dma((2, 7)),
            dma((2, 5)),
            dma((2, 5)),
            dma((12,)),
            dma((12,)),
            dma((len(REDUCE), 32)),
            dma((len(REDUCE), 32)),
            pltpu.SemaphoreType.REGULAR((4,)),
            pltpu.SemaphoreType.REGULAR((2,)),
        ],
        compiler_params=pltpu.CompilerParams(
            collective_id=0, has_side_effects=True, vmem_limit_bytes=50 * 1024 * 1024
        ),
    )(jnp.transpose(data_weight, (1, 0, 2)), blob_taps)
    return jnp.transpose(weight, (1, 0, 2)), dev[0, :3]


def solution(mesh):
    return jax.shard_map(
        shards,
        mesh=mesh,
        in_specs=(P("gy", "gz", None), P()),
        out_specs=(P("gy", "gz", None), P()),
        check_vma=False,
    )
```

```python
import functools

import jax
import jax.numpy as jnp
from jax import lax
from jax.experimental import pallas as pl
from jax.experimental.pallas import tpu as pltpu
from jax.sharding import PartitionSpec as P

MESH = pl.DeviceIdType.MESH
F32 = jnp.float32
BF16 = jnp.bfloat16

NZ, NY, NX = 20, 80, 640
DEEP = 9
G = 4
ROWS = 96
XR = 104
Y_GROUPS = ((3, 7), (7, 11), (11, 15), (15, 20), (20, 23), (23, 27), (27, 29), (0, 3))
X_GROUPS = ((0, 7, 0, 8), (7, 20, 8, 16), (20, 23, 24, 8), (23, 27, 32, 8), (27, 29, 40, 8))
XS = 48
TINY = 1e-30
X_BLOCKS = ((0, 256, 0), (256, 256, 1), (512, 128, 0))


def split(v):
    hi = v.astype(BF16)
    return hi, (v - hi.astype(F32)).astype(BF16)


def kernel(
    dw, taps, out, dev_out, p1, p2, p3, q, rh, rl, edge, w0, w1, w2, ay, stat, sx, rx,
    mine, seen,
    load_sem, oss, osr, yss, ysr, xss, xsr, iss, isr, rds, rdr, met_z, met_y,
):
    gy, gz = lax.axis_index("gy"), lax.axis_index("gz")
    ny, nz = lax.axis_size("gy"), lax.axis_size("gz")
    core = lax.rem(gz, 2)
    inner = gz + 1 - 2 * core
    outer = gz - 1 + 2 * core
    has_outer = jnp.logical_and(outer >= 0, outer < nz)
    has_up = gy < ny - 1
    has_down = gy > 0

    def plane(s):
        return core * s + (1 - core) * (NZ - 1 - s)

    barrier = pltpu.get_barrier_semaphore()
    for axis, me, size in (("gz", gz, nz), ("gy", gy, ny)):
        for far in (1, size - 1):
            pl.semaphore_signal(barrier, inc=1, device_id={axis: lax.rem(me + far, size)}, device_id_type=MESH)

    loads = [
        pltpu.make_async_copy(dw.at[plane(s)], p1.at[s + 3, 0:NY], load_sem.at[s]) for s in range(NZ)
    ]
    for copy in loads:
        copy.start()

    p1[3:34, ROWS:XR, :] = jnp.zeros((31, XR - ROWS, NX), F32)
    p1[32:34, 0:ROWS, :] = jnp.zeros((2, ROWS, NX), F32)

    @pl.when(jnp.logical_not(has_up))
    def _():
        p1[3:32, 80:88, :] = jnp.zeros((29, 8, NX), F32)
        rx[1] = jnp.zeros((XS, NX), F32)

    @pl.when(jnp.logical_not(has_down))
    def _():
        p1[3:32, 88:96, :] = jnp.zeros((29, 8, NX), F32)
        rx[0] = jnp.zeros((XS, NX), F32)

    @pl.when(jnp.logical_not(has_outer))
    def _():
        def clear(i, carry):
            p1[23 + i, 0:ROWS, :] = jnp.zeros((ROWS, NX), F32)
            return carry

        lax.fori_loop(0, DEEP, clear, 0)
        rx[0, 24:XS, :] = jnp.zeros((XS - 24, NX), F32)
        rx[1, 24:XS, :] = jnp.zeros((XS - 24, NX), F32)

    pl.semaphore_wait(barrier, 4)

    def remote(src, dst, ss, rs, where):
        return pltpu.make_async_remote_copy(
            src_ref=src, dst_ref=dst, send_sem=ss, recv_sem=rs, device_id=where, device_id_type=MESH
        )

    outs = [
        remote(dw.at[plane(19 - i)], p1.at[23 + i, 0:NY], oss.at[i], osr.at[i], {"gz": outer})
        for i in range(DEEP)
    ]

    inner_own = [
        remote(dw.at[plane(i)], p1.at[2 - i, 0:NY], iss.at[i], isr.at[i], {"gz": inner}) for i in range(3)
    ]
    def y_copies(n):
        a, b = Y_GROUPS[n]
        pa, pb = a + 3, b + 3
        up = remote(p1.at[pa:pb, 72:80], p1.at[pa:pb, 88:96], yss.at[0, n], ysr.at[0, n], {"gy": gy + 1})
        down = remote(p1.at[pa:pb, 0:8], p1.at[pa:pb, 80:88], yss.at[1, n], ysr.at[1, n], {"gy": gy - 1})
        return up, down

    def x_copies(n):
        _, _, slot, size = X_GROUPS[n]
        at = slice(slot, slot + size)
        up = remote(sx.at[0, at], rx.at[0, at], xss.at[0, n], xsr.at[0, n], {"gy": gy + 1})
        down = remote(sx.at[1, at], rx.at[1, at], xss.at[1, n], xsr.at[1, n], {"gy": gy - 1})
        return up, down

    def start_y(n):
        up, down = y_copies(n)

        @pl.when(has_up)
        def _():
            up.start()

        @pl.when(has_down)
        def _():
            down.start()

    def start_x(n):
        a, b, slot, size = X_GROUPS[n]
        for i in range(size):
            s = min(a + i, b - 1)
            sx[0, slot + i : slot + i + 1, :] = p1[s + 3, 71:72, :]
            sx[1, slot + i : slot + i + 1, :] = p1[s + 3, 8:9, :]
        up, down = x_copies(n)

        @pl.when(has_up)
        def _():
            up.start()

        @pl.when(has_down)
        def _():
            down.start()

    def wait_y(n):
        up, down = y_copies(n)

        @pl.when(has_down)
        def _():
            up.wait_recv()

        @pl.when(has_up)
        def _():
            down.wait_recv()

    def wait_x(n):
        up, down = x_copies(n)

        @pl.when(has_down)
        def _():
            up.wait_recv()

        @pl.when(has_up)
        def _():
            down.wait_recv()

        a, b, slot, size = X_GROUPS[n]
        for i in range(b - a):
            p1[a + i + 3, 96:97, :] = rx[0, slot + i : slot + i + 1, :]
            p1[a + i + 3, 97:98, :] = rx[1, slot + i : slot + i + 1, :]

    for s in range(7):
        loads[s].wait()
    start_x(0)
    start_y(7)
    start_y(0)

    @pl.when(has_outer)
    def _():
        for copy in outs:
            copy.start()

    for copy in inner_own:
        copy.start()

    for s in range(7, NZ):
        loads[s].wait()
    start_y(1)
    start_x(1)
    start_y(2)
    start_y(3)

    tv = taps[...]
    tv = tv / jnp.sum(tv, axis=1, keepdims=True)
    tv = [[tv[row : row + 1, k : k + 1] for k in range(7)] for row in range(3)]
    flip = core == 0
    kz = [jnp.where(flip, tv[1][6 - k], tv[1][k]) for k in range(7)]
    kr = [tap / kz[0] for tap in kz]

    def banded(diff):
        t = jnp.zeros(diff.shape, F32)
        for k in range(7):
            t = jnp.where(diff == k - 3, tv[2][k], t)
        return split(t)

    i = lax.broadcasted_iota(jnp.int32, (128, 128), 0)
    j = lax.broadcasted_iota(jnp.int32, (128, 128), 1)
    blocks = [banded(delta * 128 + i - j) for delta in (-1, 0, 1)]
    for w, (n0, nn, _) in zip((w0, w1, w2), X_BLOCKS):
        for part in range(3):
            for kb in range(nn // 128):
                for nb in range(nn // 128):
                    rows = slice(part * nn + kb * 128, part * nn + (kb + 1) * 128)
                    w[rows, nb * 128 : (nb + 1) * 128] = blocks[kb - nb + 1][part // 2]
        part = jnp.where(jnp.logical_or(i < 3, i >= 125), 0, jnp.where(i < 11, 1, 2))
        step = i - 8 * part
        step = jnp.where(step >= 125, step - 128, step)
        right = jnp.logical_and(step >= 0, step < (3 if n0 + nn < NX else 0))
        left = jnp.logical_and(step < 0, step >= (-3 if n0 > 0 else 0))
        for nb in range(nn // 128):
            out_lane = j + nb * 128
            diff = jnp.where(right, nn + step - out_lane, jnp.where(left, step - out_lane, 4096))
            hi, lo = banded(diff)
            w[3 * nn : 3 * nn + 128, nb * 128 : (nb + 1) * 128] = jnp.where(part == 2, lo.astype(F32), hi.astype(F32)).astype(BF16)

    o = lax.broadcasted_iota(jnp.int32, (ROWS, 128), 0)
    i = lax.broadcasted_iota(jnp.int32, (ROWS, 128), 1)
    yo = jnp.where(o < 88, o, o - 96)
    yi = jnp.where(i < 88, i, jnp.where(i < 96, i - 96, jnp.where(i == 96, -9, jnp.where(i == 97, 88, 4096))))
    diff = yi - yo + 3
    t = jnp.zeros((ROWS, 128), F32)
    for k in range(7):
        t = jnp.where(diff == k, tv[0][k] * kz[0], t)
    t_hi, t_lo = split(t)
    ay[0:ROWS, 0:128] = t_hi
    ay[0:ROWS, 128:256] = t_hi
    ay[ROWS : 2 * ROWS, 0:128] = t_lo
    ay[ROWS : 2 * ROWS, 128:256] = jnp.zeros((ROWS, 128), BF16)

    for g in range(G):
        q[g, 96:128, :] = jnp.zeros((32, NX), BF16)
        q[g, 224:256, :] = jnp.zeros((32, NX), BF16)
    for t in range(3):
        stat[t, 0] = jnp.zeros((8, 128), F32)
        stat[t, 1] = jnp.full((8, 128), 3e38, F32)

    def chunk(t, d, count=G, gate=None):
        src = (p1, p2, p3)[t]
        base = d * G
        strips = 7 if t == 0 else 6
        for strip in range(strips):
            r0 = strip * 16
            height = 8 if strip == 6 else 16
            if strip == 5 and gate is not None:
                gate()
            for lb in range(5):
                lanes = slice(lb * 128, (lb + 1) * 128)
                p = [src[base + k, r0 : r0 + height, lanes] for k in range(count + 6)]
                for g in range(count):
                    acc = p[g]
                    for k in range(1, 7):
                        acc = acc + kr[k] * p[g + k]
                    if height == 8:
                        acc = jnp.concatenate([acc, jnp.zeros((8, 128), F32)], axis=0)
                    hi, lo = split(acc)
                    q[g, r0 : r0 + 16, lanes] = hi
                    q[g, 128 + r0 : 144 + r0, lanes] = lo
        rows = 80 if t == 2 else ROWS
        for g in range(count):
            if t == 2:
                y = jnp.dot(ay[0:80, :], q[g], preferred_element_type=F32) + jnp.dot(
                    ay[ROWS : ROWS + 80, :], q[g], preferred_element_type=F32
                )
            else:
                y = jnp.dot(ay[...], q[g], preferred_element_type=F32)
                y = y[0:ROWS] + y[ROWS : 2 * ROWS]
            hi, lo = split(y)
            at = slice(g * rows, (g + 1) * rows)
            rh[at, :] = hi
            rl[at, :] = lo
            lane = lax.broadcasted_iota(jnp.int32, (rows, 128), 1)
            for e, (after, ahead) in enumerate(((2, 3), (4, 1))):
                rim = jnp.where(
                    lane < 64, y[:, after * 128 : (after + 1) * 128], y[:, ahead * 128 : (ahead + 1) * 128]
                )
                rim_hi = rim.astype(BF16).astype(F32)
                rim = jnp.where(
                    jnp.logical_or(lane < 3, lane >= 125),
                    rim_hi,
                    jnp.where(lane < 11, pltpu.roll(rim - rim_hi, 8, 1), pltpu.roll(rim_hi, 16, 1)),
                )
                edge[e, at, :] = rim.astype(BF16)
        m = count * rows
        top = jnp.zeros((8, 128), F32)
        low = jnp.full((8, 128), 3e38, F32)
        for w, (n0, nn, e) in zip((w0, w1, w2), X_BLOCKS):
            hi, lo = rh[0:m, n0 : n0 + nn], rl[0:m, n0 : n0 + nn]
            b = jnp.dot(jnp.concatenate([hi, lo, hi, edge[e, 0:m]], axis=1), w[...], preferred_element_type=F32)
            for g in range(count):
                for r0 in range(0, rows, 16):
                    for lb in range(nn // 128):
                        v = b[g * rows + r0 : g * rows + r0 + 16, lb * 128 : (lb + 1) * 128]
                        lanes = slice(n0 + lb * 128, n0 + (lb + 1) * 128)
                        if r0 < 80:
                            top = jnp.maximum(top, jnp.maximum(v[0:8], v[8:16]))
                            low = jnp.minimum(low, jnp.minimum(v[0:8], v[8:16]))
                        p = src[base + 3 + g, r0 : r0 + 16, lanes]
                        if t == 2:
                            f = p1[base + 3 + g, r0 : r0 + 16, lanes]
                            out[plane(base + g), r0 : r0 + 16, lanes] = p / (v * f)
                        else:
                            dst = (p2, p3)[t]
                            dst[base + 3 + g, r0 : r0 + 16, lanes] = p / jnp.maximum(v, TINY)
        own = jnp.int32(d) * G < NZ
        stat[t, 0] = jnp.where(own, jnp.maximum(stat[t, 0], top), stat[t, 0])
        stat[t, 1] = jnp.where(own, jnp.minimum(stat[t, 1], low), stat[t, 1])

    inner_rim = [
        remote(p1.at[3 + i, NY:XR], p1.at[2 - i, NY:XR], iss.at[3 + i], isr.at[3 + i], {"gz": inner})
        for i in range(3)
    ]
    inner_p2 = [
        remote(p2.at[3 + i], p2.at[2 - i], iss.at[6 + i], isr.at[6 + i], {"gz": inner}) for i in range(3)
    ]
    inner_p3 = [
        remote(p3.at[3 + i], p3.at[2 - i], iss.at[9 + i], isr.at[9 + i], {"gz": inner}) for i in range(3)
    ]
    def first_rims():
        wait_x(0)
        wait_y(7)
        for copy in inner_rim:
            copy.start()
        wait_y(0)
        for copy in inner_rim:
            copy.wait_recv()

    def forward(n):
        a, b = Y_GROUPS[n]
        for s in range(a, b):
            outs[s - 20].wait_recv()
        start_y(n)
        start_x(n - 2)

    def meet(k, wait):
        far = 2**k
        for axis, me, size in (("gz", gz, nz), ("gy", gy, ny)):
            if 4 * far <= size:
                sem = (met_z if axis == "gz" else met_y).at[k]
                if wait:
                    pl.semaphore_wait(sem, 2)
                else:
                    for by in (far, size - far):
                        pl.semaphore_signal(
                            sem, inc=1, device_id={axis: lax.rem(me + by, size)}, device_id_type=MESH
                        )

    def wave(d, carry):
        for k in range(5):

            @pl.when(d == k)
            def _(k=k):
                if k > 0:
                    meet(k - 1, True)
                if k < 4:
                    meet(k, False)

        for n in (1, 2, 3):

            @pl.when(d == n)
            def _(n=n):
                wait_y(n)
                if n == 1:
                    wait_x(1)

        for n in (4, 5, 6):

            @pl.when(jnp.logical_and(d == n, has_outer))
            def _(n=n):
                wait_y(n)
                wait_x(n - 2)

        @pl.when(d == 0)
        def _():
            for copy in inner_own:
                copy.wait_recv()
            chunk(0, 0, gate=first_rims)

        @pl.when(jnp.logical_and(d > 0, d < 6))
        def _():
            chunk(0, d)

        @pl.when(d == 6)
        def _():
            chunk(0, d, 2)

        @pl.when(d == 0)
        def _():
            for copy in inner_p2:
                copy.start()

        for n in (4, 5, 6):

            @pl.when(jnp.logical_and(d == n - 1, has_outer))
            def _(n=n):
                forward(n)

        @pl.when(d == 1)
        def _():
            for copy in inner_p2:
                copy.wait_recv()

        @pl.when(jnp.logical_and(d >= 1, d < 6))
        def _():
            chunk(1, d - 1)

        @pl.when(d == 6)
        def _():
            chunk(1, d - 1, 3)

        @pl.when(d == 1)
        def _():
            for copy in inner_p3:
                copy.start()

        @pl.when(d == 2)
        def _():
            for copy in inner_p3:
                copy.wait_recv()

        @pl.when(d >= 2)
        def _():
            chunk(2, d - 2)

        return carry

    lax.fori_loop(0, 7, wave, 0)

    lane = lax.broadcasted_iota(jnp.int32, (1, 128), 1)
    dev = jnp.zeros((1, 128), F32)
    for t in range(3):
        worst = jnp.maximum(jnp.max(stat[t, 0]) - 1.0, 1.0 - jnp.min(stat[t, 1]))
        dev = jnp.where(lane == t, worst, dev)

    def finish_sends():
        for copy in inner_own + inner_rim + inner_p2 + inner_p3:
            copy.wait_send()

        @pl.when(has_outer)
        def _():
            for copy in outs:
                copy.wait_send()

        def sent(copies):
            up, down = copies

            @pl.when(has_up)
            def _():
                up.wait_send()

            @pl.when(has_down)
            def _():
                down.wait_send()

        for n in (0, 1, 2, 3, 7):
            sent(y_copies(n))
        for n in range(2):
            sent(x_copies(n))

        @pl.when(has_outer)
        def _():
            for n in (4, 5, 6):
                sent(y_copies(n))
                sent(x_copies(n - 2))

    def group(stage):
        if stage == 0:
            far = [(dx, dy, dc) for dx in range(4) for dy in range(4) for dc in range(2)][1:]
            far.sort(key=lambda s: -(min(s[0], 4 - s[0]) + min(s[1], 4 - s[1])))
            x, y, c = gz // 8, lax.rem(gz // 2, 4), core
            return "gz", gz, [lax.rem(x + dx, 4) * 8 + lax.rem(y + dy, 4) * 2 + lax.rem(c + dc, 2) for dx, dy, dc in far]
        return "gy", gy, [lax.rem(gy + k, 8) for k in (4, 3, 5, 2, 6, 1, 7)]

    value = dev
    meanwhile = finish_sends
    for stage in range(2):
        axis, me, others = group(stage)
        mine[stage] = value

        def copy(k, other, slot, stage=stage, axis=axis):
            return remote(mine.at[stage], seen.at[stage, slot], rds.at[stage, k], rdr.at[stage, slot], {axis: other})

        sends = [copy(k, other, me) for k, other in enumerate(others)]
        for send in sends:
            send.start()
        seen[stage, me] = value
        meanwhile()
        for k, other in enumerate(others):
            copy(k, other, other).wait_recv()
        value = jnp.max(seen[stage, 0 : len(others) + 1], axis=0)

        def meanwhile(sends=sends):
            for send in sends:
                send.wait_send()

    dev_out[...] = value
    meanwhile()


def shards(data_weight, blob_taps):
    dma = pltpu.SemaphoreType.DMA
    weight, dev = pl.pallas_call(
        kernel,
        out_shape=(
            jax.ShapeDtypeStruct((NZ, NY, NX), F32),
            jax.ShapeDtypeStruct((1, 128), F32),
        ),
        in_specs=[pl.BlockSpec(memory_space=pl.ANY), pl.BlockSpec(memory_space=pltpu.VMEM)],
        out_specs=(pl.BlockSpec(memory_space=pltpu.VMEM), pl.BlockSpec(memory_space=pltpu.VMEM)),
        scratch_shapes=[
            pltpu.VMEM((34, XR, NX), F32),
            pltpu.VMEM((31, ROWS, NX), F32),
            pltpu.VMEM((27, ROWS, NX), F32),
            pltpu.VMEM((G, 256, NX), BF16),
            pltpu.VMEM((G * ROWS, NX), BF16),
            pltpu.VMEM((G * ROWS, NX), BF16),
            pltpu.VMEM((2, G * ROWS, 128), BF16),
            pltpu.VMEM((3 * 256 + 128, 256), BF16),
            pltpu.VMEM((3 * 256 + 128, 256), BF16),
            pltpu.VMEM((3 * 128 + 128, 128), BF16),
            pltpu.VMEM((2 * ROWS, 256), BF16),
            pltpu.VMEM((3, 2, 8, 128), F32),
            pltpu.VMEM((2, XS, NX), F32),
            pltpu.VMEM((2, XS, NX), F32),
            pltpu.VMEM((2, 1, 128), F32),
            pltpu.VMEM((2, 32, 1, 128), F32),
            dma((NZ,)),
            dma((DEEP,)),
            dma((DEEP,)),
            dma((2, 8)),
            dma((2, 8)),
            dma((2, 5)),
            dma((2, 5)),
            dma((12,)),
            dma((12,)),
            dma((2, 32)),
            dma((2, 32)),
            pltpu.SemaphoreType.REGULAR((4,)),
            pltpu.SemaphoreType.REGULAR((2,)),
        ],
        compiler_params=pltpu.CompilerParams(
            collective_id=0, has_side_effects=True, vmem_limit_bytes=50 * 1024 * 1024
        ),
    )(jnp.transpose(data_weight, (1, 0, 2)), blob_taps)
    return jnp.transpose(weight, (1, 0, 2)), dev[0, :3]


def solution(mesh):
    return jax.shard_map(
        shards,
        mesh=mesh,
        in_specs=(P("gy", "gz", None), P()),
        out_specs=(P("gy", "gz", None), P()),
        check_vma=False,
    )
```

```python
import functools

import jax
import jax.numpy as jnp
from jax import lax
from jax.experimental import pallas as pl
from jax.experimental.pallas import tpu as pltpu
from jax.sharding import PartitionSpec as P

MESH = pl.DeviceIdType.MESH
F32 = jnp.float32
BF16 = jnp.bfloat16

NZ, NY, NX = 20, 80, 640
DEEP = 9
G = 4
ROWS = 96
XR = 104
Y_GROUPS = ((3, 7), (7, 11), (11, 15), (15, 20), (20, 23), (23, 27), (27, 29), (0, 3))
X_GROUPS = ((0, 7, 0, 8), (7, 20, 8, 16), (20, 23, 24, 8), (23, 27, 32, 8), (27, 29, 40, 8))
XS = 48
TINY = 1e-30
EARLY = 4
X_BLOCKS = ((0, 256, 0), (256, 256, 1), (512, 128, 0))


def split(v):
    hi = v.astype(BF16)
    return hi, (v - hi.astype(F32)).astype(BF16)


def kernel(
    dw, taps, out, dev_out, p1, p2, p3, q, rh, rl, edge, w0, w1, w2, ay, stat, sx, rx,
    mine, seen,
    load_sem, oss, osr, yss, ysr, xss, xsr, iss, isr, rds, rdr, met_z, met_y,
):
    gy, gz = lax.axis_index("gy"), lax.axis_index("gz")
    ny, nz = lax.axis_size("gy"), lax.axis_size("gz")
    core = lax.rem(gz, 2)
    inner = gz + 1 - 2 * core
    outer = gz - 1 + 2 * core
    has_outer = jnp.logical_and(outer >= 0, outer < nz)
    has_up = gy < ny - 1
    has_down = gy > 0

    def plane(s):
        return core * s + (1 - core) * (NZ - 1 - s)

    barrier = pltpu.get_barrier_semaphore()
    for axis, me, size in (("gz", gz, nz), ("gy", gy, ny)):
        for far in (1, size - 1):
            pl.semaphore_signal(barrier, inc=1, device_id={axis: lax.rem(me + far, size)}, device_id_type=MESH)

    loads = [
        pltpu.make_async_copy(dw.at[plane(s)], p1.at[s + 3, 0:NY], load_sem.at[s]) for s in range(NZ)
    ]
    for copy in loads:
        copy.start()

    p1[3:34, ROWS:XR, :] = jnp.zeros((31, XR - ROWS, NX), F32)
    p1[32:34, 0:ROWS, :] = jnp.zeros((2, ROWS, NX), F32)

    @pl.when(jnp.logical_not(has_up))
    def _():
        p1[3:32, 80:88, :] = jnp.zeros((29, 8, NX), F32)
        rx[1] = jnp.zeros((XS, NX), F32)

    @pl.when(jnp.logical_not(has_down))
    def _():
        p1[3:32, 88:96, :] = jnp.zeros((29, 8, NX), F32)
        rx[0] = jnp.zeros((XS, NX), F32)

    @pl.when(jnp.logical_not(has_outer))
    def _():
        def clear(i, carry):
            p1[23 + i, 0:ROWS, :] = jnp.zeros((ROWS, NX), F32)
            return carry

        lax.fori_loop(0, DEEP, clear, 0)
        rx[0, 24:XS, :] = jnp.zeros((XS - 24, NX), F32)
        rx[1, 24:XS, :] = jnp.zeros((XS - 24, NX), F32)

    pl.semaphore_wait(barrier, 4)

    def remote(src, dst, ss, rs, where):
        return pltpu.make_async_remote_copy(
            src_ref=src, dst_ref=dst, send_sem=ss, recv_sem=rs, device_id=where, device_id_type=MESH
        )

    outs = [
        remote(dw.at[plane(19 - i)], p1.at[23 + i, 0:NY], oss.at[i], osr.at[i], {"gz": outer})
        for i in range(DEEP)
    ]

    inner_own = [
        remote(dw.at[plane(i)], p1.at[2 - i, 0:NY], iss.at[i], isr.at[i], {"gz": inner}) for i in range(3)
    ]
    def y_copies(n):
        a, b = Y_GROUPS[n]
        pa, pb = a + 3, b + 3
        up = remote(p1.at[pa:pb, 72:80], p1.at[pa:pb, 88:96], yss.at[0, n], ysr.at[0, n], {"gy": gy + 1})
        down = remote(p1.at[pa:pb, 0:8], p1.at[pa:pb, 80:88], yss.at[1, n], ysr.at[1, n], {"gy": gy - 1})
        return up, down

    def x_copies(n):
        _, _, slot, size = X_GROUPS[n]
        at = slice(slot, slot + size)
        up = remote(sx.at[0, at], rx.at[0, at], xss.at[0, n], xsr.at[0, n], {"gy": gy + 1})
        down = remote(sx.at[1, at], rx.at[1, at], xss.at[1, n], xsr.at[1, n], {"gy": gy - 1})
        return up, down

    def start_y(n):
        up, down = y_copies(n)

        @pl.when(has_up)
        def _():
            up.start()

        @pl.when(has_down)
        def _():
            down.start()

    def start_x(n):
        a, b, slot, size = X_GROUPS[n]
        for i in range(size):
            s = min(a + i, b - 1)
            sx[0, slot + i : slot + i + 1, :] = p1[s + 3, 71:72, :]
            sx[1, slot + i : slot + i + 1, :] = p1[s + 3, 8:9, :]
        up, down = x_copies(n)

        @pl.when(has_up)
        def _():
            up.start()

        @pl.when(has_down)
        def _():
            down.start()

    def wait_y(n):
        up, down = y_copies(n)

        @pl.when(has_down)
        def _():
            up.wait_recv()

        @pl.when(has_up)
        def _():
            down.wait_recv()

    def wait_x(n):
        up, down = x_copies(n)

        @pl.when(has_down)
        def _():
            up.wait_recv()

        @pl.when(has_up)
        def _():
            down.wait_recv()

        a, b, slot, size = X_GROUPS[n]
        for i in range(b - a):
            p1[a + i + 3, 96:97, :] = rx[0, slot + i : slot + i + 1, :]
            p1[a + i + 3, 97:98, :] = rx[1, slot + i : slot + i + 1, :]

    for s in range(7):
        loads[s].wait()
    start_x(0)
    start_y(7)
    start_y(0)

    @pl.when(has_outer)
    def _():
        for copy in outs:
            copy.start()

    for copy in inner_own:
        copy.start()

    for s in range(7, NZ):
        loads[s].wait()
    start_y(1)
    start_x(1)
    start_y(2)
    start_y(3)

    tv = taps[...]
    tv = tv / jnp.sum(tv, axis=1, keepdims=True)
    tv = [[tv[row : row + 1, k : k + 1] for k in range(7)] for row in range(3)]
    flip = core == 0
    kz = [jnp.where(flip, tv[1][6 - k], tv[1][k]) for k in range(7)]
    kr = [tap / kz[0] for tap in kz]

    def banded(diff):
        t = jnp.zeros(diff.shape, F32)
        for k in range(7):
            t = jnp.where(diff == k - 3, tv[2][k], t)
        return split(t)

    i = lax.broadcasted_iota(jnp.int32, (128, 128), 0)
    j = lax.broadcasted_iota(jnp.int32, (128, 128), 1)
    blocks = [banded(delta * 128 + i - j) for delta in (-1, 0, 1)]
    for w, (n0, nn, _) in zip((w0, w1, w2), X_BLOCKS):
        for part in range(3):
            for kb in range(nn // 128):
                for nb in range(nn // 128):
                    rows = slice(part * nn + kb * 128, part * nn + (kb + 1) * 128)
                    w[rows, nb * 128 : (nb + 1) * 128] = blocks[kb - nb + 1][part // 2]
        part = jnp.where(jnp.logical_or(i < 3, i >= 125), 0, jnp.where(i < 11, 1, 2))
        step = i - 8 * part
        step = jnp.where(step >= 125, step - 128, step)
        right = jnp.logical_and(step >= 0, step < (3 if n0 + nn < NX else 0))
        left = jnp.logical_and(step < 0, step >= (-3 if n0 > 0 else 0))
        for nb in range(nn // 128):
            out_lane = j + nb * 128
            diff = jnp.where(right, nn + step - out_lane, jnp.where(left, step - out_lane, 4096))
            hi, lo = banded(diff)
            w[3 * nn : 3 * nn + 128, nb * 128 : (nb + 1) * 128] = jnp.where(part == 2, lo.astype(F32), hi.astype(F32)).astype(BF16)

    o = lax.broadcasted_iota(jnp.int32, (ROWS, 128), 0)
    i = lax.broadcasted_iota(jnp.int32, (ROWS, 128), 1)
    yo = jnp.where(o < 88, o, o - 96)
    yi = jnp.where(i < 88, i, jnp.where(i < 96, i - 96, jnp.where(i == 96, -9, jnp.where(i == 97, 88, 4096))))
    diff = yi - yo + 3
    t = jnp.zeros((ROWS, 128), F32)
    for k in range(7):
        t = jnp.where(diff == k, tv[0][k] * kz[0], t)
    t_hi, t_lo = split(t)
    ay[0:ROWS, 0:128] = t_hi
    ay[0:ROWS, 128:256] = t_hi
    ay[ROWS : 2 * ROWS, 0:128] = t_lo
    ay[ROWS : 2 * ROWS, 128:256] = jnp.zeros((ROWS, 128), BF16)

    def clear_q(g, carry):
        q[g, 96:128, :] = jnp.zeros((32, NX), BF16)
        q[g, 224:256, :] = jnp.zeros((32, NX), BF16)
        return carry

    lax.fori_loop(0, EARLY * G, clear_q, 0)
    for t in range(3):
        stat[t, 0] = jnp.zeros((8, 128), F32)
        stat[t, 1] = jnp.full((8, 128), 3e38, F32)

    def smear_z(t, base, strips, count, qb):
        src = (p1, p2, p3)[t]
        for strip in strips:
            r0 = strip * 16
            height = 8 if strip == 6 else 16
            for lb in range(5):
                lanes = slice(lb * 128, (lb + 1) * 128)
                p = [src[base + k, r0 : r0 + height, lanes] for k in range(count + 6)]
                for g in range(count):
                    acc = p[g]
                    for k in range(1, 7):
                        acc = acc + kr[k] * p[g + k]
                    if height == 8:
                        acc = jnp.concatenate([acc, jnp.zeros((8, 128), F32)], axis=0)
                    hi, lo = split(acc)
                    q[qb + g, r0 : r0 + 16, lanes] = hi
                    q[qb + g, 128 + r0 : 144 + r0, lanes] = lo

    def chunk(t, d, count=G, early=False):
        src = (p1, p2, p3)[t]
        base = d * G
        qb = base if early else 0
        smear_z(t, base, range(5 if early else 0, 7 if t == 0 else 6), count, qb)
        rows = 80 if t == 2 else ROWS
        for g in range(count):
            if t == 2:
                y = jnp.dot(ay[0:80, :], q[qb + g], preferred_element_type=F32) + jnp.dot(
                    ay[ROWS : ROWS + 80, :], q[qb + g], preferred_element_type=F32
                )
            else:
                y = jnp.dot(ay[...], q[qb + g], preferred_element_type=F32)
                y = y[0:ROWS] + y[ROWS : 2 * ROWS]
            hi, lo = split(y)
            at = slice(g * rows, (g + 1) * rows)
            rh[at, :] = hi
            rl[at, :] = lo
            lane = lax.broadcasted_iota(jnp.int32, (rows, 128), 1)
            for e, (after, ahead) in enumerate(((2, 3), (4, 1))):
                rim = jnp.where(
                    lane < 64, y[:, after * 128 : (after + 1) * 128], y[:, ahead * 128 : (ahead + 1) * 128]
                )
                rim_hi = rim.astype(BF16).astype(F32)
                rim = jnp.where(
                    jnp.logical_or(lane < 3, lane >= 125),
                    rim_hi,
                    jnp.where(lane < 11, pltpu.roll(rim - rim_hi, 8, 1), pltpu.roll(rim_hi, 16, 1)),
                )
                edge[e, at, :] = rim.astype(BF16)
        m = count * rows
        top = jnp.zeros((8, 128), F32)
        low = jnp.full((8, 128), 3e38, F32)
        for w, (n0, nn, e) in zip((w0, w1, w2), X_BLOCKS):
            hi, lo = rh[0:m, n0 : n0 + nn], rl[0:m, n0 : n0 + nn]
            b = jnp.dot(jnp.concatenate([hi, lo, hi, edge[e, 0:m]], axis=1), w[...], preferred_element_type=F32)
            for g in range(count):
                for r0 in range(0, rows, 16):
                    for lb in range(nn // 128):
                        v = b[g * rows + r0 : g * rows + r0 + 16, lb * 128 : (lb + 1) * 128]
                        lanes = slice(n0 + lb * 128, n0 + (lb + 1) * 128)
                        if r0 < 80:
                            top = jnp.maximum(top, jnp.maximum(v[0:8], v[8:16]))
                            low = jnp.minimum(low, jnp.minimum(v[0:8], v[8:16]))
                        p = src[base + 3 + g, r0 : r0 + 16, lanes]
                        if t == 2:
                            f = p1[base + 3 + g, r0 : r0 + 16, lanes]
                            out[plane(base + g), r0 : r0 + 16, lanes] = p / (v * f)
                        else:
                            dst = (p2, p3)[t]
                            dst[base + 3 + g, r0 : r0 + 16, lanes] = p / jnp.maximum(v, TINY)
        own = jnp.int32(d) * G < NZ
        stat[t, 0] = jnp.where(own, jnp.maximum(stat[t, 0], top), stat[t, 0])
        stat[t, 1] = jnp.where(own, jnp.minimum(stat[t, 1], low), stat[t, 1])

    inner_rim = [
        remote(p1.at[3 + i, NY:XR], p1.at[2 - i, NY:XR], iss.at[3 + i], isr.at[3 + i], {"gz": inner})
        for i in range(3)
    ]
    inner_p2 = [
        remote(p2.at[3 + i], p2.at[2 - i], iss.at[6 + i], isr.at[6 + i], {"gz": inner}) for i in range(3)
    ]
    inner_p3 = [
        remote(p3.at[3 + i], p3.at[2 - i], iss.at[9 + i], isr.at[9 + i], {"gz": inner}) for i in range(3)
    ]
    def first_rims():
        wait_x(0)
        wait_y(7)
        for copy in inner_rim:
            copy.start()
        wait_y(0)
        for copy in inner_rim:
            copy.wait_recv()

    def forward(n):
        a, b = Y_GROUPS[n]
        for s in range(a, b):
            outs[s - 20].wait_recv()
        start_y(n)
        start_x(n - 2)

    def meet(k, wait):
        far = 2**k
        for axis, me, size in (("gz", gz, nz), ("gy", gy, ny)):
            if 4 * far <= size:
                sem = (met_z if axis == "gz" else met_y).at[k]
                if wait:
                    pl.semaphore_wait(sem, 2)
                else:
                    for by in (far, size - far):
                        pl.semaphore_signal(
                            sem, inc=1, device_id={axis: lax.rem(me + by, size)}, device_id_type=MESH
                        )

    def wave(d, carry):
        for k in range(5):

            @pl.when(d == k)
            def _(k=k):
                if k > 0:
                    meet(k - 1, True)
                if k < 4:
                    meet(k, False)

        @pl.when(d == 0)
        def _():
            first_rims()

        for n in (1, 2, 3):

            @pl.when(d == n)
            def _(n=n):
                wait_y(n)
                if n == 1:
                    wait_x(1)

        for n in (4, 5, 6):

            @pl.when(jnp.logical_and(d == n, has_outer))
            def _(n=n):
                wait_y(n)
                wait_x(n - 2)

        @pl.when(d < EARLY)
        def _():
            chunk(0, d, early=True)

        @pl.when(jnp.logical_and(d >= EARLY, d < 6))
        def _():
            chunk(0, d)

        @pl.when(d == 6)
        def _():
            chunk(0, d, 2)

        @pl.when(d == 0)
        def _():
            for copy in inner_p2:
                copy.start()

        for n in (4, 5, 6):

            @pl.when(jnp.logical_and(d == n - 1, has_outer))
            def _(n=n):
                forward(n)

        @pl.when(d == 1)
        def _():
            for copy in inner_p2:
                copy.wait_recv()

        @pl.when(jnp.logical_and(d >= 1, d < 6))
        def _():
            chunk(1, d - 1)

        @pl.when(d == 6)
        def _():
            chunk(1, d - 1, 3)

        @pl.when(d == 1)
        def _():
            for copy in inner_p3:
                copy.start()

        @pl.when(d == 2)
        def _():
            for copy in inner_p3:
                copy.wait_recv()

        @pl.when(d >= 2)
        def _():
            chunk(2, d - 2)

        return carry

    for copy in inner_own:
        copy.wait_recv()

    def own_rows(d, carry):
        smear_z(0, d * G, range(5), G, d * G)
        return carry

    lax.fori_loop(0, EARLY, own_rows, 0)
    lax.fori_loop(0, 7, wave, 0)

    lane = lax.broadcasted_iota(jnp.int32, (1, 128), 1)
    dev = jnp.zeros((1, 128), F32)
    for t in range(3):
        worst = jnp.maximum(jnp.max(stat[t, 0]) - 1.0, 1.0 - jnp.min(stat[t, 1]))
        dev = jnp.where(lane == t, worst, dev)

    def finish_sends():
        for copy in inner_own + inner_rim + inner_p2 + inner_p3:
            copy.wait_send()

        @pl.when(has_outer)
        def _():
            for copy in outs:
                copy.wait_send()

        def sent(copies):
            up, down = copies

            @pl.when(has_up)
            def _():
                up.wait_send()

            @pl.when(has_down)
            def _():
                down.wait_send()

        for n in (0, 1, 2, 3, 7):
            sent(y_copies(n))
        for n in range(2):
            sent(x_copies(n))

        @pl.when(has_outer)
        def _():
            for n in (4, 5, 6):
                sent(y_copies(n))
                sent(x_copies(n - 2))

    def group(stage):
        if stage == 0:
            far = [(dx, dy, dc) for dx in range(4) for dy in range(4) for dc in range(2)][1:]
            far.sort(key=lambda s: -(min(s[0], 4 - s[0]) + min(s[1], 4 - s[1])))
            x, y, c = gz // 8, lax.rem(gz // 2, 4), core
            return "gz", gz, [lax.rem(x + dx, 4) * 8 + lax.rem(y + dy, 4) * 2 + lax.rem(c + dc, 2) for dx, dy, dc in far]
        return "gy", gy, [lax.rem(gy + k, 8) for k in (4, 3, 5, 2, 6, 1, 7)]

    value = dev
    meanwhile = finish_sends
    for stage in range(2):
        axis, me, others = group(stage)
        mine[stage] = value

        def copy(k, other, slot, stage=stage, axis=axis):
            return remote(mine.at[stage], seen.at[stage, slot], rds.at[stage, k], rdr.at[stage, slot], {axis: other})

        sends = [copy(k, other, me) for k, other in enumerate(others)]
        for send in sends:
            send.start()
        seen[stage, me] = value
        meanwhile()
        for k, other in enumerate(others):
            copy(k, other, other).wait_recv()
        value = jnp.max(seen[stage, 0 : len(others) + 1], axis=0)

        def meanwhile(sends=sends):
            for send in sends:
                send.wait_send()

    dev_out[...] = value
    meanwhile()


def shards(data_weight, blob_taps):
    dma = pltpu.SemaphoreType.DMA
    weight, dev = pl.pallas_call(
        kernel,
        out_shape=(
            jax.ShapeDtypeStruct((NZ, NY, NX), F32),
            jax.ShapeDtypeStruct((1, 128), F32),
        ),
        in_specs=[pl.BlockSpec(memory_space=pl.ANY), pl.BlockSpec(memory_space=pltpu.VMEM)],
        out_specs=(pl.BlockSpec(memory_space=pltpu.VMEM), pl.BlockSpec(memory_space=pltpu.VMEM)),
        scratch_shapes=[
            pltpu.VMEM((34, XR, NX), F32),
            pltpu.VMEM((31, ROWS, NX), F32),
            pltpu.VMEM((27, ROWS, NX), F32),
            pltpu.VMEM((EARLY * G, 256, NX), BF16),
            pltpu.VMEM((G * ROWS, NX), BF16),
            pltpu.VMEM((G * ROWS, NX), BF16),
            pltpu.VMEM((2, G * ROWS, 128), BF16),
            pltpu.VMEM((3 * 256 + 128, 256), BF16),
            pltpu.VMEM((3 * 256 + 128, 256), BF16),
            pltpu.VMEM((3 * 128 + 128, 128), BF16),
            pltpu.VMEM((2 * ROWS, 256), BF16),
            pltpu.VMEM((3, 2, 8, 128), F32),
            pltpu.VMEM((2, XS, NX), F32),
            pltpu.VMEM((2, XS, NX), F32),
            pltpu.VMEM((2, 1, 128), F32),
            pltpu.VMEM((2, 32, 1, 128), F32),
            dma((NZ,)),
            dma((DEEP,)),
            dma((DEEP,)),
            dma((2, 8)),
            dma((2, 8)),
            dma((2, 5)),
            dma((2, 5)),
            dma((12,)),
            dma((12,)),
            dma((2, 32)),
            dma((2, 32)),
            pltpu.SemaphoreType.REGULAR((4,)),
            pltpu.SemaphoreType.REGULAR((2,)),
        ],
        compiler_params=pltpu.CompilerParams(
            collective_id=0, has_side_effects=True, vmem_limit_bytes=50 * 1024 * 1024
        ),
    )(jnp.transpose(data_weight, (1, 0, 2)), blob_taps)
    return jnp.transpose(weight, (1, 0, 2)), dev[0, :3]


def solution(mesh):
    return jax.shard_map(
        shards,
        mesh=mesh,
        in_specs=(P("gy", "gz", None), P()),
        out_specs=(P("gy", "gz", None), P()),
        check_vma=False,
    )
```
